32 devices in a mesh: row: 8 (over z, core), col: 4 (over y, x).
Axes of the slice: x: 2, y: 2, z: 4, core: 2. Of those that a mesh axis runs over, the one named last changes fastest.
Arguments:
- matrix: float32 [12288, 12288], P('row', 'col'), may hold values from -8 to 8
Outputs:
- updated: float32 [12288, 12288], P('row', 'col')
- reflectors: float32 [16, 12288], replicated
- coefficients: float32 [2, 16], replicated
The draws below stay inside these ranges and needn't reach their ends.
All inputs are finite; a program needn't handle non-finite values.
Results may differ from the reference program's by a relative error of at most 0.0003.
Values sent between devices are 32-bit elements; how exact they have to be, the bound alone decides.
A program may use at most 64 MiB of HBM per device.

```python
import jax
import jax.numpy as jnp
from jax import lax

ORDER = 12288
PANEL_COLUMNS = 16


def draw_matrix(key, part):
    first = jax.random.fold_in(jax.random.fold_in(key, 11), 0)
    raw = jax.random.normal(first, (ORDER, ORDER), jnp.float32)
    sym = (raw + raw.T) * jnp.float32(0.7071067811865476)
    return jnp.clip(sym, -8.0, 8.0)


def setup_inputs(seed: int = 0) -> dict:
    splits = jax.random.split(jax.random.key(seed), 2)
    return {
        "matrix": draw_matrix(jax.random.fold_in(splits[1], 71), 0),
    }


HIGH = lax.Precision.HIGHEST

def reference(matrix):
    order = matrix.shape[0]
    positions = jnp.arange(order, dtype=jnp.int32)
    reflectors = jnp.zeros((PANEL_COLUMNS, order), jnp.float32)
    reflected_images = jnp.zeros((PANEL_COLUMNS, order), jnp.float32)
    reflector_scales = []
    below_diagonal = []
    for step in range(PANEL_COLUMNS):
        column = matrix[:, step] - jnp.dot(reflected_images[:, step], reflectors, precision=HIGH) - jnp.dot(reflectors[:, step], reflected_images, precision=HIGH)
        below = jnp.where(positions > step, column, 0.0)
        leading = column[step + 1]
        norm_value = jnp.sqrt(jnp.sum(below * below))
        reflector = jnp.where(positions == step + 1, 1.0, below / (leading + norm_value))
        reflector_scale = 1.0 + leading / norm_value
        product = jnp.dot(matrix, reflector, precision=HIGH)
        images_dot = jnp.dot(reflected_images, reflector, precision=HIGH)
        reflect_dot = jnp.dot(reflectors, reflector, precision=HIGH)
        image = reflector_scale * (product - jnp.dot(images_dot, reflectors, precision=HIGH) - jnp.dot(reflect_dot, reflected_images, precision=HIGH))
        image = image - 0.5 * reflector_scale * jnp.sum(image * reflector) * reflector
        reflectors = reflectors.at[step].set(reflector)
        reflected_images = reflected_images.at[step].set(image)
        reflector_scales.append(reflector_scale)
        below_diagonal.append(-norm_value)
    left_side = jnp.concatenate([reflectors, reflected_images], axis=0)
    right_side = jnp.concatenate([reflected_images, reflectors], axis=0)
    updated = matrix - jnp.einsum('kr,kc->rc', left_side, right_side, precision=HIGH)
    coefficients = jnp.stack([jnp.stack(reflector_scales), jnp.stack(below_diagonal)])
    return (updated, reflectors, coefficients)
```

```python
import jax
import jax.numpy as jnp
from jax import lax
from jax.experimental import pallas as pl
from jax.experimental.pallas import tpu as pltpu
from jax.sharding import PartitionSpec as P

K = 16
PAIRS = K // 2
HEAD = 24
LANES = 128
SUB = 8
GROUPS = LANES // SUB
MESH = pl.DeviceIdType.MESH
F32 = jnp.float32


def lanes_of(t):
    return slice(t * LANES, (t + 1) * LANES)


def spread_row(row):
    return jnp.broadcast_to(row, (LANES, LANES)).T


def panel_kernel(rows, cols, n_row, n_col, mat, tile, refl, vwr, vwc, coef,
                 headrows, phead, rowc, vout,
                 sum_a, sum_b, sc_a, sc_b, red_a, red_b, hd_a, hd_b,
                 c0r, ur, pr, aur, c0c, uc, pc, auc, c0h, uh, ph, auh, vwh,
                 coefc, coefp, vuwu, scal, b0r, b0c, xs, accs, dacc,
                 load_sem, hrow_sem, head_sem, row_sem, v_sem,
                 ya_sem, sa_sem, ra_sem, ha_sem, yb_sem, sb_sem, rb_sem, hb_sem,
                 ssem):
    halves = cols // rows
    r = lax.axis_index("row")
    c = lax.axis_index("col")
    blocks = rows // LANES
    ctiles = cols // LANES
    rtiles = rows // LANES
    half_tiles = ctiles // 2
    half_blocks = blocks // 2
    diag = r // halves == c
    own_half = lax.rem(r, halves)

    def along_row(dr):
        return (lax.rem(r + dr, n_row), c)

    def along_col(dc):
        return (r, lax.rem(c + dc, n_col))

    def remote(src, dst, sem, device):
        return pltpu.make_async_remote_copy(src, dst, ssem, sem, device_id=device, device_id_type=MESH)

    def landed(ref, sem):
        pltpu.make_async_copy(ref, ref, sem).wait()

    def to_rows(ref, sem):
        for dr in range(1, n_row):
            remote(ref, ref, sem, along_row(dr)).start()

    def to_cols(ref, sem):
        for dc in range(1, n_col):
            remote(ref, ref, sem, along_col(dc)).start()

    def chunk(i):
        part = pl.ds(pl.multiple_of(i * LANES, LANES), LANES)
        return pltpu.make_async_copy(mat.at[part], tile.at[part], load_sem.at[i])

    hrow_copy = pltpu.make_async_copy(mat.at[0:HEAD], headrows, hrow_sem)
    pl.when(r == 0)(lambda: hrow_copy.start())

    def start_chunk(i, carry):
        chunk(i).start()
        return carry

    lax.fori_loop(0, blocks, start_chunk, 0)

    barrier = pltpu.get_barrier_semaphore()
    for dr in range(n_row):
        for dc in range(n_col):
            if dr or dc:
                pl.semaphore_signal(barrier, inc=1, device_id=(lax.rem(r + dr, n_row), lax.rem(c + dc, n_col)),
                                    device_id_type=MESH)

    for ref in (vwr, vwc, vwh, c0r, ur, pr, aur, uc, pc, auc, c0h, uh, ph, auh, coefc, coefp, vuwu, scal, dacc, coef):
        ref[...] = jnp.zeros_like(ref)

    @pl.when(r == 0)
    def _():
        hrow_copy.wait()
        rowc[0] = headrows[0:1, :]
        rowc[1] = headrows[1:2, :]

    pl.semaphore_wait(barrier, n_row * n_col - 1)

    @pl.when(r == 0)
    def _():
        to_rows(rowc.at[0:2], row_sem.at[0])

        @pl.when(c == 0)
        def _():
            phead[...] = headrows[:, 0:LANES]
            for dr in range(n_row):
                for dc in range(n_col):
                    if dr or dc:
                        remote(headrows.at[:, 0:LANES], phead, head_sem,
                               (lax.rem(r + dr, n_row), lax.rem(c + dc, n_col))).start()

    @pl.when(r != 0)
    def _():
        landed(rowc.at[0:2], row_sem.at[0])

    c0c[...] = rowc[0]

    lane_r = lax.broadcasted_iota(jnp.int32, (1, rows), 1)
    lane_c = lax.broadcasted_iota(jnp.int32, (1, cols), 1)
    l128 = lax.broadcasted_iota(jnp.int32, (1, LANES), 1)
    pos_r = lane_r + r * rows
    pos_c = lane_c + c * cols
    k16 = lax.broadcasted_iota(jnp.int32, (K, LANES), 0)
    s40 = lax.broadcasted_iota(jnp.int32, (2 * K + SUB, LANES), 0)
    t40 = lax.broadcasted_iota(jnp.int32, (2 * K + SUB, LANES), 1)
    eye40 = s40 == t40
    diag3 = (lax.broadcasted_iota(jnp.int32, (GROUPS, SUB, LANES), 0) * SUB
             + lax.broadcasted_iota(jnp.int32, (GROUPS, SUB, LANES), 1)
             == lax.broadcasted_iota(jnp.int32, (GROUPS, SUB, LANES), 2))

    def srow(k):
        return scal[k:k + 1, :]

    def wide(x, n):
        return x if n == 1 else jnp.concatenate([x] * n, axis=1)

    def advance(j, vw, c0, u, p, au_ref, au_new, row_new, pos):
        tau, kap, e, inv = srow(0), srow(1), srow(2), srow(3)
        cc = coefc[...]
        cp = coefp[...]
        hot = jnp.where(j >= 0, j + 1, -1)
        last = jnp.maximum(j, 0)
        wrow, vrow, prow = [], [], []
        for t in range(c0.shape[1] // LANES):
            sl = lanes_of(t)
            x = vw[:, sl]
            au = au_new(t)
            row = row_new(t)
            ta = tau * au
            c0n = row - ta + jnp.sum(x * cc, axis=0, keepdims=True)
            pn = ta - jnp.sum(x * cp, axis=0, keepdims=True)
            u_old = u[:, sl]
            un = jnp.where(pos[:, sl] > j + 1, (c0[:, sl] + e * u_old) * inv, 0.0)
            un = jnp.where(pos[:, sl] == hot, 1.0, un)
            wrow.append(p[:, sl] - kap * u_old)
            vrow.append(un)
            prow.append(pn)
            c0[:, sl] = c0n
            u[:, sl] = un
            p[:, sl] = pn
            au_ref[:, sl] = au
        vw[pl.ds(K + j - 1, 1), :] = jnp.concatenate(wrow, axis=1)
        vw[pl.ds(last, 1), :] = jnp.concatenate(vrow, axis=1)
        vw[pl.ds(K + j, 1), :] = jnp.concatenate(prow, axis=1)

    def dots_add(vw, x_ref, u, p, t):
        sl = pl.ds(pl.multiple_of(t * LANES, LANES), LANES)
        x = x_ref[:, sl]
        dacc[0:2 * K, :] += vw[:, sl] * x
        dacc[2 * K:2 * K + 1, :] += x * x
        dacc[2 * K + 1:2 * K + 2, :] += u[:, sl] * p[:, sl]

    def dots_row():
        d = jnp.sum(dacc[...], axis=1, keepdims=True)
        out = jnp.sum(jnp.where(eye40, d, 0.0), axis=0, keepdims=True)
        dacc[...] = jnp.zeros_like(dacc)
        return out

    def matvec_cols(i, j):
        b0c[...] = jnp.where(pos_c > j + 1, c0c[...], 0.0)
        xb = [jnp.broadcast_to(b0c[:, lanes_of(t)], (SUB, LANES)) for t in range(ctiles)]
        per = ctiles // half_blocks

        def reduce_block(k):
            part = pl.ds(pl.multiple_of(k * LANES, LANES), LANES)
            a = accs[part, :].reshape(GROUPS, SUB, LANES)
            s = jnp.sum(a, axis=2, keepdims=True)
            row = jnp.sum(jnp.sum(jnp.where(diag3, s, 0.0), axis=0), axis=0, keepdims=True)
            sum_b[i, c, :, pl.ds(pl.multiple_of(k * LANES, LANES), LANES)] = row

        def block(first):
            def body(k, carry):
                pl.when(i == 0)(lambda: chunk(k).wait())
                part = pl.ds(pl.multiple_of(k * LANES, LANES), LANES)
                reduce_block(jnp.maximum(k - 1, 0))
                acc = jnp.zeros((GROUPS, SUB, LANES), F32)
                for t in range(ctiles):
                    acc = acc + tile[part, lanes_of(t)].reshape(GROUPS, SUB, LANES) * xb[t][None]
                accs[part, :] = acc.reshape(LANES, LANES)
                if first:
                    for q in range(per):
                        dots_add(vwc, b0c, uc, pc, k * per + q)
                return carry
            return body

        lax.fori_loop(0, half_blocks, block(True), 0)
        sc_b[i, c] = dots_row()
        to_cols(sc_b.at[i, c], sb_sem.at[i])
        lax.fori_loop(half_blocks, blocks, block(False), 0)
        reduce_block(blocks - 1)
        to_cols(sum_b.at[i, c], yb_sem.at[i])

    def matvec_rows(i, j):
        b0r[...] = jnp.where(pos_r > j + 1, c0r[...], 0.0)

        def spread(k):
            return spread_row(b0r[:, pl.ds(pl.multiple_of(k * LANES, LANES), LANES)])

        zero = jnp.zeros((SUB, LANES), F32)

        def products(part, bc, accs_in, base):
            b3 = bc.reshape(GROUPS, SUB, LANES)
            out = []
            for t in range(half_tiles):
                x = tile[part, lanes_of(base + t)].reshape(GROUPS, SUB, LANES)
                out.append(accs_in[t] + jnp.sum(x * b3, axis=0))
            return tuple(out)

        def first(k, state):
            bc, acc = state
            part = pl.ds(pl.multiple_of(k * LANES, LANES), LANES)
            nxt = spread(jnp.minimum(k + 1, blocks - 1))
            xs[part, :] = bc
            dots_add(vwr, b0r, ur, pr, k)
            return nxt, products(part, bc, acc, 0)

        def second(k, acc):
            part = pl.ds(pl.multiple_of(k * LANES, LANES), LANES)
            return products(part, xs[part, :], acc, half_tiles)

        def store(acc, base):
            for t in range(half_tiles):
                sum_a[i, r, base // half_tiles, :, lanes_of(t)] = jnp.sum(acc[t], axis=0, keepdims=True)

        _, acc = lax.fori_loop(0, blocks, first, (spread(0), (zero,) * half_tiles))
        store(acc, 0)
        sc_a[i, r] = dots_row()
        to_rows(sc_a.at[i, r], sa_sem.at[i])
        to_rows(sum_a.at[i, r, 0], ya_sem.at[i, 0])
        acc = lax.fori_loop(0, blocks, second, (zero,) * half_tiles)
        store(acc, half_tiles)
        to_rows(sum_a.at[i, r, 1], ya_sem.at[i, 1])

    def head_advance(j, auh_row):
        advance(j, vwh, c0h, uh, ph, auh, lambda t: auh_row, lambda t: phead[pl.ds(j + 1, 1), :], l128)

    def lane_pick(x, index):
        s = jnp.sum(jnp.where(l128 == index, x, 0.0), axis=1, keepdims=True)
        return jnp.broadcast_to(s, x.shape)

    def picks(j):
        head = vwh[...]
        return (lane_pick(head, j), lane_pick(head, j + 1), lane_pick(c0h[...], j + 1),
                lane_pick(uh[...], j + 1), lane_pick(ph[...], j))

    def scalars(j, sc, picked):
        hj, hj1, c0h1, uj1, pent = picked
        d = jnp.sum(jnp.where(eye40, jnp.broadcast_to(sc, eye40.shape), 0.0), axis=1, keepdims=True)
        d = jnp.broadcast_to(d, eye40.shape)
        vb, wb = d[0:K], d[K:2 * K]
        n0, kp = d[2 * K:2 * K + 1], d[2 * K + 1:2 * K + 2]
        hjv, hjw, hj1v, hj1w = hj[0:K], hj[K:2 * K], hj1[0:K], hj1[K:2 * K]
        last = k16 == j - 1
        tau_prev, bb_prev = srow(0), srow(4)
        kap = 0.5 * tau_prev * kp
        e = 2.0 * kap - pent
        lead = c0h1 + e * uj1
        n1 = jnp.sum(jnp.where(last, vb, 0.0), axis=0, keepdims=True)
        b2 = jnp.maximum(n0 + e * (2.0 * n1 + e * (bb_prev - uj1 * uj1)), 0.0)
        sig = jnp.sqrt(b2 + lead * lead)
        inv = 1.0 / (lead + sig)
        tau = 1.0 + lead / sig
        lk = jnp.where(last, kap, 0.0)
        hjw = hjw - lk * hjv
        hj1w = hj1w - lk * hj1v
        uu = bb_prev + 1.0
        vup = jnp.where(last, uu, vuwu[0:K, :])
        wup = jnp.where(last, kp - kap * uu, vuwu[K:2 * K, :])
        wb = wb - lk * vb
        vu = (vb + e * (vup - hjv - uj1 * hj1v)) * inv + hj1v
        wu = (wb + e * (wup - hjw - uj1 * hj1w)) * inv + hj1w
        beta = tau * vu - hj1v
        alpha = tau * wu - hj1w - lk * beta
        delta = tau * vu
        gamma = tau * wu - lk * delta
        coefc[0:K, :] = alpha
        coefc[K:2 * K, :] = beta
        coefp[0:K, :] = gamma
        coefp[K:2 * K, :] = delta
        vuwu[0:K, :] = vu
        vuwu[K:2 * K, :] = wu
        scal[0:1, :] = tau
        scal[1:2, :] = kap
        scal[2:3, :] = e
        scal[3:4, :] = inv
        scal[4:5, :] = b2 * inv * inv
        scal[5:6, :] = uj1
        coef[0:1, :] = jnp.where(l128 == j, tau, coef[0:1, :])
        coef[1:2, :] = jnp.where(l128 == j, -sig, coef[1:2, :])

    def finish(j, vw, c0, u, p, au_ref, total, row, row_next, pos):
        def au_new(t):
            e, inv, uj1 = srow(2), srow(3), srow(5)
            nxt = row_next(t)
            aq = au_ref[:, lanes_of(t)] - row(t) - uj1 * nxt
            return (total(t) + e * aq) * inv + nxt
        advance(j, vw, c0, u, p, au_ref, au_new, row_next, pos)

    def slot_sum(read, n):
        acc = read(0)
        for s in range(1, n):
            acc = acc + read(s)
        return acc

    def send_v(k, i):
        vout[k, c] = uc[...]
        to_cols(vout.at[k, c], v_sem.at[i])

    def pack_v(i):
        landed(vout.at[0:2, 0:n_col - 1], v_sem.at[i])

    def place_v(i):
        for q in range(2):
            refl[pl.ds(2 * i + q, 1), :] = jnp.concatenate([vout[2 * i + q, cc] for cc in range(n_col)], axis=1)

    def send_red_b(i, j):
        @pl.when(diag)
        def _():
            piece = pl.ds(pl.multiple_of(own_half * rows, LANES), rows)
            red_b[i, 0] = auc[:, piece]
            red_b[i, 1] = rowc[j, :, piece]
            red_b[i, 2] = rowc[j + 1, :, piece]
            to_cols(red_b.at[i], rb_sem.at[i])

    def step_cols(i):
        j = 2 * i
        send_red_b(i, j)

        @pl.when(c == 0)
        def _():
            hd_b[i] = auc[:, 0:LANES]
            to_cols(hd_b.at[i], hb_sem.at[i])

        @pl.when(r == 0)
        def _():
            rowc[j + 2] = headrows[pl.ds(j + 2, 1), :]
            rowc[j + 3] = headrows[pl.ds(j + 3, 1), :]
            to_rows(rowc.at[pl.ds(j + 2, 2)], row_sem.at[i + 1])

        matvec_cols(i, j)

        @pl.when(jnp.logical_and(i == 0, jnp.logical_or(r != 0, c != 0)))
        def _():
            landed(phead, head_sem)

        pl.when(c != 0)(lambda: landed(hd_b.at[i], hb_sem.at[i]))
        head_advance(j - 1, hd_b[i])
        picked = picks(j)
        pl.when(jnp.logical_not(diag))(lambda: landed(red_b.at[i], rb_sem.at[i]))
        advance(j - 1, vwr, c0r, ur, pr, aur, lambda t: red_b[i, 0, :, lanes_of(t)],
                lambda t: red_b[i, 1, :, lanes_of(t)], pos_r)
        landed(sc_b.at[i, 0:n_col - 1], sb_sem.at[i])
        scalars(j, slot_sum(lambda s: sc_b[i, s], n_col), picked)
        landed(sum_b.at[i, 0:n_col - 1], yb_sem.at[i])
        finish(j, vwr, c0r, ur, pr, aur, lambda t: slot_sum(lambda s: sum_b[i, s, :, lanes_of(t)], n_col),
               lambda t: red_b[i, 1, :, lanes_of(t)], lambda t: red_b[i, 2, :, lanes_of(t)], pos_r)

    def step_rows(i):
        j = 2 * i + 1

        @pl.when(diag)
        def _():
            red_a[i, own_half] = aur[...]
            to_rows(red_a.at[i, own_half], ra_sem.at[i, own_half])

        @pl.when(r == 0)
        def _():
            hd_a[i] = aur[:, 0:LANES]
            to_rows(hd_a.at[i], ha_sem.at[i])

        matvec_rows(i, j)

        pl.when(r != 0)(lambda: landed(hd_a.at[i], ha_sem.at[i]))
        head_advance(j - 1, hd_a[i])
        picked = picks(j)
        for h in range(halves):
            pl.when(r != halves * c + h)(lambda h=h: landed(red_a.at[i, h], ra_sem.at[i, h]))
        advance(j - 1, vwc, c0c, uc, pc, auc,
                lambda t: red_a[i, t // rtiles, :, lanes_of(t % rtiles)],
                lambda t: rowc[j, :, lanes_of(t)], pos_c)
        send_v(j - 1, i)

        @pl.when(i > 0)
        def _():
            pack_v(i - 1)
            place_v(i - 1)

        landed(sc_a.at[i, 0:n_row - 1], sa_sem.at[i])
        scalars(j, slot_sum(lambda s: sc_a[i, s], n_row), picked)
        pl.when(r != 0)(lambda: landed(rowc.at[0:2], row_sem.at[i + 1]))
        for h in range(2):
            landed(sum_a.at[i, 0:n_row - 1, 0], ya_sem.at[i, h])
        finish(j, vwc, c0c, uc, pc, auc,
               lambda t: slot_sum(lambda s: sum_a[i, s, t // half_tiles, :, lanes_of(t % half_tiles)], n_row),
               lambda t: rowc[j, :, lanes_of(t)], lambda t: rowc[j + 1, :, lanes_of(t)], pos_c)
        send_v(j, i)

    def pair(i, carry):
        step_cols(i)
        step_rows(i)
        return carry

    lax.fori_loop(0, PAIRS, pair, 0)

    f = PAIRS

    @pl.when(diag)
    def _():
        piece = pl.ds(pl.multiple_of(own_half * rows, LANES), rows)
        red_b[f, 0] = auc[:, piece]
        to_cols(red_b.at[f, 0:1], rb_sem.at[f])

    kp = jnp.sum(uc[...] * pc[...], axis=1, keepdims=True)
    sc_b[f, c] = jnp.broadcast_to(kp, (1, LANES))
    to_cols(sc_b.at[f, c], sb_sem.at[f])
    pl.when(jnp.logical_not(diag))(lambda: landed(red_b.at[f, 0:1], rb_sem.at[f]))
    advance(K - 1, vwr, c0r, ur, pr, aur, lambda t: red_b[f, 0, :, lanes_of(t)],
            lambda t: red_b[f, 0, :, lanes_of(t)], pos_r)
    landed(sc_b.at[f, 0:n_col - 1], sb_sem.at[f])
    kap = 0.5 * srow(0) * slot_sum(lambda s: sc_b[f, s], n_col)
    vwr[2 * K - 1:2 * K, :] = pr[...] - wide(kap, rtiles) * ur[...]
    vwc[2 * K - 1:2 * K, :] = pc[...] - wide(kap, ctiles) * uc[...]
    pack_v(PAIRS - 1)
    place_v(PAIRS - 1)

    def drain(i, carry):
        landed(sum_a.at[i, 0:n_row - 1], ssem)
        landed(sc_a.at[i, 0:n_row - 1], ssem)
        landed(sum_b.at[i, 0:n_col - 1], ssem)
        landed(sc_b.at[i, 0:n_col - 1], ssem)
        for dc in range(1, n_col):
            landed(vout.at[0:2, 0], ssem)

        @pl.when(diag)
        def _():
            for dr in range(1, n_row):
                landed(red_a.at[i, 0], ssem)
            for dc in range(1, n_col):
                landed(red_b.at[i], ssem)

        @pl.when(c == 0)
        def _():
            for dc in range(1, n_col):
                landed(hd_b.at[i], ssem)

        @pl.when(r == 0)
        def _():
            for dr in range(1, n_row):
                landed(hd_a.at[i], ssem)
                landed(rowc.at[0:2], ssem)
        return carry

    lax.fori_loop(0, PAIRS, drain, 0)
    landed(sc_b.at[f, 0:n_col - 1], ssem)

    @pl.when(diag)
    def _():
        for dc in range(1, n_col):
            landed(red_b.at[f, 0:1], ssem)

    @pl.when(r == 0)
    def _():
        for dr in range(1, n_row):
            landed(rowc.at[0:2], ssem)

        @pl.when(c == 0)
        def _():
            for d in range(1, n_row * n_col):
                landed(phead, ssem)


def pieces(x):
    hi = x.astype(jnp.bfloat16)
    rest = x - hi.astype(F32)
    mid = rest.astype(jnp.bfloat16)
    low = (rest - mid.astype(F32)).astype(jnp.bfloat16)
    return hi, mid, low


def update_kernel(rows, cols, tile, vwr, vwc, out, left, right, buf, sem):
    blocks = rows // LANES
    order = ((0, 0), (0, 1), (1, 0), (1, 1), (0, 2), (2, 0))
    two = 2 * K
    lp = pieces(vwr[...])
    wv = jnp.concatenate([vwc[K:two, :], vwc[0:K, :]], axis=0)
    rp = pieces(wv)
    for q, (a, b) in enumerate(order):
        left[q * two:(q + 1) * two, :] = lp[a]
        right[q * two:(q + 1) * two, :] = rp[b]

    def body(i, carry):
        part = pl.ds(pl.multiple_of(i * LANES, LANES), LANES)
        lt = left[:, part]
        change = lax.dot_general(lt, right[...], (((0,), (0,)), ((), ())), preferred_element_type=F32)
        buf[part, :] = tile[part, :] - change
        pltpu.make_async_copy(buf.at[part], out.at[part], sem).start()
        return carry

    lax.fori_loop(0, blocks, body, 0)
    pltpu.make_async_copy(buf, out, sem).wait()


def make_per_device(n_row, n_col):
    def per_device(matrix):
        rows, cols = matrix.shape
        halves = cols // rows
        f32 = F32
        vmem = pl.BlockSpec(memory_space=pltpu.VMEM)
        anyspace = pl.BlockSpec(memory_space=pl.ANY)
        dma = pltpu.SemaphoreType.DMA
        full = n_row * rows

        def kernel(*refs):
            panel_kernel(rows, cols, n_row, n_col, *refs)

        def vm(*shape):
            return pltpu.VMEM(shape, f32)

        tile, refl, vwr, vwc, coef = pl.pallas_call(
            kernel,
            out_shape=(
                jax.ShapeDtypeStruct((rows, cols), f32),
                jax.ShapeDtypeStruct((K, full), f32),
                jax.ShapeDtypeStruct((2 * K, rows), f32),
                jax.ShapeDtypeStruct((2 * K, cols), f32),
                jax.ShapeDtypeStruct((2, LANES), f32),
            ),
            in_specs=[anyspace],
            out_specs=(vmem,) * 5,
            scratch_shapes=[
                vm(HEAD, cols), vm(HEAD, LANES), vm(K + 2, 1, cols), vm(K, n_col, 1, cols),
                vm(PAIRS, n_row, 2, 1, cols // 2), vm(PAIRS, n_col, 1, rows),
                vm(PAIRS, n_row, 1, LANES), vm(PAIRS + 1, n_col, 1, LANES),
                vm(PAIRS, halves, 1, rows), vm(PAIRS + 1, 3, 1, rows),
                vm(PAIRS, 1, LANES), vm(PAIRS, 1, LANES),
                vm(1, rows), vm(1, rows), vm(1, rows), vm(1, rows),
                vm(1, cols), vm(1, cols), vm(1, cols), vm(1, cols),
                vm(1, LANES), vm(1, LANES), vm(1, LANES), vm(1, LANES), vm(2 * K, LANES),
                vm(2 * K, LANES), vm(2 * K, LANES), vm(2 * K, LANES), vm(8, LANES),
                vm(1, rows), vm(1, cols), vm(rows, LANES), vm(rows, LANES), vm(2 * K + SUB, LANES),
                dma((rows // LANES,)), dma, dma, dma((PAIRS + 1,)), dma((PAIRS,)),
                dma((PAIRS, 2)), dma((PAIRS,)), dma((PAIRS, halves)), dma((PAIRS,)),
                dma((PAIRS,)), dma((PAIRS + 1,)), dma((PAIRS + 1,)), dma((PAIRS,)),
                dma,
            ],
            compiler_params=pltpu.CompilerParams(
                collective_id=0, has_side_effects=True, vmem_limit_bytes=24 * 1024 * 1024),
        )(matrix)

        def update(*refs):
            update_kernel(rows, cols, *refs)

        updated = pl.pallas_call(
            update,
            out_shape=jax.ShapeDtypeStruct((rows, cols), f32),
            in_specs=[vmem] * 3,
            out_specs=anyspace,
            scratch_shapes=[
                pltpu.VMEM((12 * K, rows), jnp.bfloat16),
                pltpu.VMEM((12 * K, cols), jnp.bfloat16),
                vm(rows, cols),
                dma,
            ],
            compiler_params=pltpu.CompilerParams(vmem_limit_bytes=24 * 1024 * 1024),
        )(tile, vwr, vwc)
        return updated, refl, coef[:, :K]
    return per_device


def solution(mesh):
    return jax.shard_map(
        make_per_device(mesh.shape["row"], mesh.shape["col"]),
        mesh=mesh,
        in_specs=(P("row", "col"),),
        out_specs=(P("row", "col"), P(), P()),
        check_vma=False,
    )
```

```python
import jax
import jax.numpy as jnp
from jax import lax
from jax.experimental import pallas as pl
from jax.experimental.pallas import tpu as pltpu
from jax.sharding import PartitionSpec as P

K = 16
PAIRS = K // 2
HEAD = 24
LANES = 128
SUB = 8
GROUPS = LANES // SUB
BATCH = 4
STEP = 3
MESH = pl.DeviceIdType.MESH
F32 = jnp.float32


def lanes_of(t):
    return slice(t * LANES, (t + 1) * LANES)


def tile_rows(n):
    return -(-n // SUB) * SUB


def spread_row(row):
    return jnp.broadcast_to(row, (LANES, LANES)).T


def panel_kernel(rows, cols, n_row, n_col, mat, tile, refl, vwr, vwc, coef,
                 headrows, phead, rowc, vout,
                 sum_a, sum_b, sc_a, sc_b, red_a, red_b, hd_a, hd_b,
                 wr, c0r, ur, pr, aur, qr, wc, c0c, uc, pc, auc, qc, wh, c0h, uh, ph, auh,
                 coefc, coefp, vuwu, scal, b0r, b0c, xs, accs, dacc,
                 load_sem, hrow_sem, head_sem, row_sem, v_sem,
                 ya_sem, sa_sem, ra_sem, ha_sem, yb_sem, sb_sem, rb_sem, hb_sem,
                 ssem):
    halves = cols // rows
    r = lax.axis_index("row")
    c = lax.axis_index("col")
    blocks = rows // LANES
    ctiles = cols // LANES
    rt = rows // LANES
    rp = tile_rows(rt)
    half_blocks = blocks // 2
    diag = r // halves == c
    own_half = lax.rem(r, halves)

    def along_row(dr):
        return (lax.rem(r + dr, n_row), c)

    def along_col(dc):
        return (r, lax.rem(c + dc, n_col))

    def remote(src, dst, sem, device):
        return pltpu.make_async_remote_copy(src, dst, ssem, sem, device_id=device, device_id_type=MESH)

    def landed(ref, sem):
        pltpu.make_async_copy(ref, ref, sem).wait()

    def to_rows(ref, sem):
        for dr in range(1, n_row):
            remote(ref, ref, sem, along_row(dr)).start()

    def to_cols(ref, sem):
        for dc in range(1, n_col):
            remote(ref, ref, sem, along_col(dc)).start()

    def block_rows(k):
        return pl.ds(pl.multiple_of(k * LANES, LANES), LANES)

    def chunk(i):
        part = block_rows(i)
        return pltpu.make_async_copy(mat.at[part], tile.at[part], load_sem.at[i])

    hrow_copy = pltpu.make_async_copy(mat.at[0:HEAD], headrows, hrow_sem)
    pl.when(r == 0)(lambda: hrow_copy.start())

    def start_chunk(i, carry):
        chunk(i).start()
        return carry

    lax.fori_loop(0, blocks, start_chunk, 0)

    barrier = pltpu.get_barrier_semaphore()
    for dr in range(1, n_row):
        pl.semaphore_signal(barrier, inc=1, device_id=along_row(dr), device_id_type=MESH)
    for dc in range(1, n_col):
        pl.semaphore_signal(barrier, inc=1, device_id=along_col(dc), device_id_type=MESH)

    for ref in (wr, c0r, ur, pr, aur, wc, uc, pc, auc, wh, c0h, uh, ph, auh, coefc, coefp, vuwu, scal, coef, vwr, vwc):
        ref[...] = jnp.zeros_like(ref)
    if rp > rt:
        for ref in (rowc, sum_a, sum_b, red_a, red_b):
            lead = ref.shape[:-2]
            ref[tuple(slice(None) for _ in lead) + (slice(rt, rp),)] = jnp.zeros(lead + (rp - rt, LANES), F32)

    def take_row(k):
        x = headrows[pl.ds(k, 1), :]
        for t in range(ctiles):
            rowc[k, t // rt, t % rt:t % rt + 1, :] = x[:, lanes_of(t)]

    @pl.when(r == 0)
    def _():
        hrow_copy.wait()
        take_row(0)
        take_row(1)

    pl.semaphore_wait(barrier, n_row + n_col - 2)

    @pl.when(r == 0)
    def _():
        to_rows(rowc.at[0:2, :, 0:rt], row_sem.at[0])

        @pl.when(c == 0)
        def _():
            phead[...] = headrows[:, 0:LANES]
            for dr in range(1, n_row):
                remote(headrows.at[:, 0:LANES], phead, head_sem, along_row(dr)).start()

    @pl.when(r != 0)
    def _():
        landed(rowc.at[0:2, :, 0:rt], row_sem.at[0])

    def positions(n, base):
        shape = (n, rp, LANES)
        t = lax.broadcasted_iota(jnp.int32, shape, 1)
        x = (lax.broadcasted_iota(jnp.int32, shape, 0) * rt + t) * LANES + lax.broadcasted_iota(jnp.int32, shape, 2)
        return jnp.where(t < rt, x + base, -2)

    l128 = lax.broadcasted_iota(jnp.int32, (1, LANES), 1)
    pos_r = positions(1, r * rows)
    pos_c = positions(halves, c * cols)
    pos_h = jnp.where(lax.broadcasted_iota(jnp.int32, (1, SUB, LANES), 1) < 1,
                      lax.broadcasted_iota(jnp.int32, (1, SUB, LANES), 2), -2)
    k16 = lax.broadcasted_iota(jnp.int32, (K, LANES), 0)
    s40 = lax.broadcasted_iota(jnp.int32, (2 * K + SUB, LANES), 0)
    t40 = lax.broadcasted_iota(jnp.int32, (2 * K + SUB, LANES), 1)
    eye40 = s40 == t40
    diag3 = (lax.broadcasted_iota(jnp.int32, (GROUPS, SUB, LANES), 0) * SUB
             + lax.broadcasted_iota(jnp.int32, (GROUPS, SUB, LANES), 1)
             == lax.broadcasted_iota(jnp.int32, (GROUPS, SUB, LANES), 2))

    def srow(k):
        return scal[k:k + 1, :]

    def splat(ref, k, like):
        return jnp.broadcast_to(ref[k:k + 1, :], like.shape[1:])[None]

    def weighted(w, ref, like):
        acc = w[0] * splat(ref, 0, like)
        for k in range(1, 2 * K):
            acc = acc + w[k] * splat(ref, k, like)
        return acc

    def record(j, w, c0, u, p, au_ref, au, c0n, pn, pos):
        kap, e, inv = splat(scal, 1, pos), splat(scal, 2, pos), splat(scal, 3, pos)
        hot = jnp.where(j >= 0, j + 1, -1)
        u_old = u[...]
        un = jnp.where(pos > j + 1, (c0[...] + e * u_old) * inv, 0.0)
        un = jnp.where(pos == hot, 1.0, un)
        fixed = p[...] - kap * u_old
        w[K + j - 1] = fixed
        w[jnp.maximum(j, 0)] = un
        w[K + j] = pn
        c0[...] = c0n
        u[...] = un
        p[...] = pn
        au_ref[...] = au

    def advance(j, w, c0, u, p, au_ref, au, row, pos):
        ta = splat(scal, 0, pos) * au
        c0n = row - ta + weighted(w, coefc, pos)
        pn = ta - weighted(w, coefp, pos)
        record(j, w, c0, u, p, au_ref, au, c0n, pn, pos)

    def finish(j, w, c0, u, p, au_ref, q, total, row, row_next, pos, b0):
        tau, kap, e, inv, uj1 = (splat(scal, k, pos) for k in (0, 1, 2, 3, 5))
        aq = au_ref[...] - row - uj1 * row_next
        au = (total + e * aq) * inv + row_next
        pn = tau * au - weighted(w, coefp, pos)
        c0n = q[...] + (2.0 * kap * uj1) * u[...] - pn
        record(j, w, c0, u, p, au_ref, au, c0n, pn, pos)
        prepare(j + 1, w, u, p, c0n, b0, pos)

    def fold(x):
        y = x.reshape(-1, SUB, LANES)
        acc = y[0]
        for k in range(1, y.shape[0]):
            acc = acc + y[k]
        return acc

    def prepare(j, w, u, p, c0n, b0, pos):
        x = jnp.where(pos > j + 1, c0n, 0.0)
        b0[...] = x
        for k in range(2 * K):
            dacc[k] = fold(w[k] * x)
        dacc[2 * K] = fold(x * x)
        dacc[2 * K + 1] = fold(u[...] * p[...])

    def dots_row():
        acc = jnp.zeros((SUB, LANES), F32)
        for k in range(2 * K + 2):
            s = jnp.sum(dacc[k], axis=1, keepdims=True)
            acc = jnp.where(jnp.broadcast_to(l128, (SUB, LANES)) == k, s, acc)
        return jnp.sum(acc, axis=0, keepdims=True)

    def matvec_cols(i, j):
        xb = [jnp.broadcast_to(b0c[t // rt, t % rt:t % rt + 1, :], (SUB, LANES)) for t in range(ctiles)]

        def reduce_block(k):
            a = accs[block_rows(k), :].reshape(GROUPS, SUB, LANES)
            s = jnp.sum(a, axis=2, keepdims=True)
            row = jnp.sum(jnp.sum(jnp.where(diag3, s, 0.0), axis=0), axis=0, keepdims=True)
            sum_b[i, c, pl.ds(k, 1), :] = row

        def block(first):
            def body(q, carry):
                for s in range(STEP):
                    pl.when(i == 0)(lambda s=s: chunk(q * STEP + s).wait())
                for s in range(STEP):
                    reduce_block(jnp.maximum(q - 1, 0) * STEP + s)
                if first:
                    sc_b[i, c] = dots_row()
                for s in range(STEP):
                    k = q * STEP + s
                    for g in range(0, GROUPS, BATCH):
                        piece = pl.ds(pl.multiple_of(k * LANES + g * SUB, SUB), BATCH * SUB)
                        acc = jnp.zeros((BATCH, SUB, LANES), F32)
                        for t in range(ctiles):
                            acc = acc + tile[piece, lanes_of(t)].reshape(BATCH, SUB, LANES) * xb[t][None]
                        accs[piece, :] = acc.reshape(BATCH * SUB, LANES)
                return carry
            return body

        lax.fori_loop(0, half_blocks // STEP, block(True), 0)
        to_cols(sc_b.at[i, c], sb_sem.at[i])
        lax.fori_loop(half_blocks // STEP, blocks // STEP, block(False), 0)
        for s in range(STEP):
            reduce_block(blocks - STEP + s)
        to_cols(sum_b.at[i, c, 0:rt], yb_sem.at[i])

    def spread(k):
        xs[block_rows(k), :] = spread_row(b0r[0, pl.ds(k, 1), :])

    def spread_first():
        for s in range(STEP):
            spread(s)

    def matvec_rows(i, j):
        zero = jnp.zeros((SUB, LANES), F32)

        def products(k, accs_in, base):
            out = list(accs_in)
            for g in range(GROUPS):
                piece = pl.ds(pl.multiple_of(k * LANES + g * SUB, SUB), SUB)
                b = xs[piece, :]
                for t in range(rt):
                    out[t] = out[t] + tile[piece, lanes_of(base + t)] * b
            return tuple(out)

        def sweep(h):
            def body(q, acc):
                for s in range(STEP):
                    acc = products(q * STEP + s, acc, h * rt)
                if h == 0:
                    for s in range(STEP):
                        spread(jnp.minimum((q + 1) * STEP + s, blocks - 1))
                    sc_a[i, r] = dots_row()
                return acc
            return body

        for h in range(halves):
            acc = lax.fori_loop(0, blocks // STEP, sweep(h), (zero,) * rt)
            for t in range(rt):
                sum_a[i, r, h, t:t + 1, :] = jnp.sum(acc[t], axis=0, keepdims=True)
            if h == 0:
                to_rows(sc_a.at[i, r], sa_sem.at[i])
            to_rows(sum_a.at[i, r, h, 0:rt], ya_sem.at[i, h])

    def head_advance(j, auh_row):
        advance(j, wh, c0h, uh, ph, auh, auh_row, phead[pl.ds(j + 1, 1), :][None] * jnp.ones((1, SUB, 1), F32), pos_h)

    def lane_pick(x, index):
        s = jnp.sum(jnp.where(l128 == index, x, 0.0), axis=1, keepdims=True)
        return jnp.broadcast_to(s, x.shape)

    def picks(j):
        head = wh[:, 0, 0, :]
        return (lane_pick(head, j), lane_pick(head, j + 1), lane_pick(c0h[0, 0:1, :], j + 1),
                lane_pick(uh[0, 0:1, :], j + 1), lane_pick(ph[0, 0:1, :], j))

    def pre_q(w, q, picked, row_next, pos):
        hj1 = picked[1]
        coefc[0:K, :] = hj1[K:2 * K]
        coefc[K:2 * K, :] = hj1[0:K]
        q[...] = row_next - weighted(w, coefc, pos)

    def scalars(j, sc, picked):
        hj, hj1, c0h1, uj1, pent = picked
        d = jnp.sum(jnp.where(eye40, jnp.broadcast_to(sc, eye40.shape), 0.0), axis=1, keepdims=True)
        d = jnp.broadcast_to(d, eye40.shape)
        vb, wb = d[0:K], d[K:2 * K]
        n0, kp = d[2 * K:2 * K + 1], d[2 * K + 1:2 * K + 2]
        hjv, hjw, hj1v, hj1w = hj[0:K], hj[K:2 * K], hj1[0:K], hj1[K:2 * K]
        last = k16 == j - 1
        tau_prev, bb_prev = srow(0), srow(4)
        kap = 0.5 * tau_prev * kp
        e = 2.0 * kap - pent
        lead = c0h1 + e * uj1
        n1 = jnp.sum(jnp.where(last, vb, 0.0), axis=0, keepdims=True)
        b2 = jnp.maximum(n0 + e * (2.0 * n1 + e * (bb_prev - uj1 * uj1)), 0.0)
        sig = jnp.sqrt(b2 + lead * lead)
        inv = 1.0 / (lead + sig)
        tau = 1.0 + lead / sig
        lk = jnp.where(last, kap, 0.0)
        hjw = hjw - lk * hjv
        hj1w = hj1w - lk * hj1v
        uu = bb_prev + 1.0
        vup = jnp.where(last, uu, vuwu[0:K, :])
        wup = jnp.where(last, kp - kap * uu, vuwu[K:2 * K, :])
        wb = wb - lk * vb
        vu = (vb + e * (vup - hjv - uj1 * hj1v)) * inv + hj1v
        wu = (wb + e * (wup - hjw - uj1 * hj1w)) * inv + hj1w
        beta = tau * vu - hj1v
        alpha = tau * wu - hj1w - lk * beta
        delta = tau * vu
        gamma = tau * wu - lk * delta
        coefc[0:K, :] = alpha
        coefc[K:2 * K, :] = beta
        coefp[0:K, :] = gamma
        coefp[K:2 * K, :] = delta
        vuwu[0:K, :] = vu
        vuwu[K:2 * K, :] = wu
        scal[0:1, :] = tau
        scal[1:2, :] = kap
        scal[2:3, :] = e
        scal[3:4, :] = inv
        scal[4:5, :] = b2 * inv * inv
        scal[5:6, :] = uj1
        coef[0:1, :] = jnp.where(l128 == j, tau, coef[0:1, :])
        coef[1:2, :] = jnp.where(l128 == j, -sig, coef[1:2, :])

    def slot_sum(read, n):
        acc = read(0)
        for s in range(1, n):
            acc = acc + read(s)
        return acc

    def flat(ref):
        n = ref.shape[0]
        return jnp.concatenate([ref[h, t:t + 1, :] for h in range(n) for t in range(rt)], axis=1)

    def send_v(k, i):
        vout[k, c] = uc[...]
        to_cols(vout.at[k, c, :, 0:rt], v_sem.at[i])

    def place_v(i):
        landed(vout.at[0:2, 0:n_col - 1, :, 0:rt], v_sem.at[i])
        for q in range(2):
            refl[pl.ds(2 * i + q, 1), :] = jnp.concatenate(
                [flat(vout.at[2 * i + q, s]) for s in range(n_col)], axis=1)

    def flat_v(k, w, out):
        out[pl.ds(k, 1), :] = flat(w.at[k])

    def send_au_b(i, count, j):
        @pl.when(diag)
        def _():
            red_b[i, 0] = auc[own_half]
            for q in range(1, count):
                red_b[i, q] = rowc[j + q - 1, own_half]
            to_cols(red_b.at[i, 0:count, 0:rt], rb_sem.at[i])

    def step_cols(i):
        j = 2 * i
        send_au_b(i, 3, j)

        @pl.when(c == 0)
        def _():
            hd_b[i] = auc[0:1, 0:SUB]
            to_cols(hd_b.at[i], hb_sem.at[i])

            @pl.when(i == 0)
            def _():
                pl.when(r != 0)(lambda: landed(phead, head_sem))
                to_cols(phead, head_sem)

        matvec_cols(i, j)

        @pl.when(r == 0)
        def _():
            take_row(j + 2)
            take_row(j + 3)
            to_rows(rowc.at[pl.ds(j + 2, 2), :, 0:rt], row_sem.at[i + 1])

        @pl.when(jnp.logical_and(i == 0, c != 0))
        def _():
            landed(phead, head_sem)

        pl.when(c != 0)(lambda: landed(hd_b.at[i], hb_sem.at[i]))
        head_advance(j - 1, hd_b[i])
        picked = picks(j)
        pl.when(jnp.logical_not(diag))(lambda: landed(red_b.at[i, :, 0:rt], rb_sem.at[i]))
        advance(j - 1, wr, c0r, ur, pr, aur, red_b[i, 0:1], red_b[i, 1:2], pos_r)
        pre_q(wr, qr, picked, red_b[i, 2:3], pos_r)
        landed(sc_b.at[i, 0:n_col - 1], sb_sem.at[i])
        scalars(j, slot_sum(lambda s: sc_b[i, s], n_col), picked)
        landed(sum_b.at[i, 0:n_col - 1, 0:rt], yb_sem.at[i])
        finish(j, wr, c0r, ur, pr, aur, qr, slot_sum(lambda s: sum_b[i, s], n_col)[None],
               red_b[i, 1:2], red_b[i, 2:3], pos_r, b0r)
        spread_first()

    def step_rows(i):
        j = 2 * i + 1

        @pl.when(diag)
        def _():
            red_a[i, own_half] = aur[0]
            to_rows(red_a.at[i, own_half, 0:rt], ra_sem.at[i, own_half])

        @pl.when(r == 0)
        def _():
            hd_a[i] = aur[0:1, 0:SUB]
            to_rows(hd_a.at[i], ha_sem.at[i])

        matvec_rows(i, j)

        pl.when(r != 0)(lambda: landed(hd_a.at[i], ha_sem.at[i]))
        head_advance(j - 1, hd_a[i])
        picked = picks(j)
        for h in range(halves):
            pl.when(r != halves * c + h)(lambda h=h: landed(red_a.at[i, h, 0:rt], ra_sem.at[i, h]))
        pl.when(r != 0)(lambda: landed(rowc.at[0:2, :, 0:rt], row_sem.at[i + 1]))
        advance(j - 1, wc, c0c, uc, pc, auc, red_a[i], rowc[j], pos_c)
        pre_q(wc, qc, picked, rowc[j + 1], pos_c)
        send_v(j - 1, i)
        pl.when(i > 0)(lambda: place_v(i - 1))
        landed(sc_a.at[i, 0:n_row - 1], sa_sem.at[i])
        scalars(j, slot_sum(lambda s: sc_a[i, s], n_row), picked)
        for h in range(halves):
            landed(sum_a.at[i, 0:n_row - 1, 0, 0:rt], ya_sem.at[i, h])
        finish(j, wc, c0c, uc, pc, auc, qc, slot_sum(lambda s: sum_a[i, s], n_row),
               rowc[j], rowc[j + 1], pos_c, b0c)
        send_v(j, i)

    def pair(i, carry):
        step_cols(i)
        step_rows(i)
        return carry

    c0c[...] = rowc[0]
    prepare(0, wc, uc, pc, rowc[0], b0c, pos_c)
    lax.fori_loop(0, PAIRS, pair, 0)

    f = PAIRS
    send_au_b(f, 1, K)
    kp = jnp.sum(dacc[2 * K + 1], axis=1, keepdims=True)
    sc_b[f, c] = jnp.sum(jnp.broadcast_to(kp, (SUB, LANES)), axis=0, keepdims=True)
    to_cols(sc_b.at[f, c], sb_sem.at[f])
    for k in range(2 * K - 1):
        flat_v(k, wc, vwc)
    for k in range(2 * K - 2):
        if k != K - 1:
            flat_v(k, wr, vwr)
    pl.when(jnp.logical_not(diag))(lambda: landed(red_b.at[f, 0:1, 0:rt], rb_sem.at[f]))
    advance(K - 1, wr, c0r, ur, pr, aur, red_b[f, 0:1], red_b[f, 0:1], pos_r)
    flat_v(K - 1, wr, vwr)
    flat_v(2 * K - 2, wr, vwr)
    landed(sc_b.at[f, 0:n_col - 1], sb_sem.at[f])
    kap = 0.5 * srow(0) * slot_sum(lambda s: sc_b[f, s], n_col)
    wr[2 * K - 1] = pr[...] - jnp.broadcast_to(kap, (rp, LANES))[None] * ur[...]
    wc[2 * K - 1] = pc[...] - jnp.broadcast_to(kap, (rp, LANES))[None] * uc[...]
    flat_v(2 * K - 1, wr, vwr)
    flat_v(2 * K - 1, wc, vwc)
    place_v(PAIRS - 1)

    def drain(i, carry):
        landed(sum_a.at[i, 0:n_row - 1, :, 0:rt], ssem)
        landed(sc_a.at[i, 0:n_row - 1], ssem)
        landed(sum_b.at[i, 0:n_col - 1, 0:rt], ssem)
        landed(sc_b.at[i, 0:n_col - 1], ssem)
        landed(vout.at[0:2, 0:n_col - 1, :, 0:rt], ssem)

        @pl.when(diag)
        def _():
            for dr in range(1, n_row):
                landed(red_a.at[i, 0, 0:rt], ssem)
            for dc in range(1, n_col):
                landed(red_b.at[i, :, 0:rt], ssem)

        @pl.when(c == 0)
        def _():
            for dc in range(1, n_col):
                landed(hd_b.at[i], ssem)

        @pl.when(r == 0)
        def _():
            for dr in range(1, n_row):
                landed(hd_a.at[i], ssem)
                landed(rowc.at[0:2, :, 0:rt], ssem)
        return carry

    lax.fori_loop(0, PAIRS, drain, 0)
    landed(sc_b.at[f, 0:n_col - 1], ssem)

    @pl.when(diag)
    def _():
        for dc in range(1, n_col):
            landed(red_b.at[f, 0:1, 0:rt], ssem)

    @pl.when(r == 0)
    def _():
        for dr in range(1, n_row):
            landed(rowc.at[0:2, :, 0:rt], ssem)

    @pl.when(c == 0)
    def _():
        for dc in range(1, n_col):
            landed(phead, ssem)

        @pl.when(r == 0)
        def _():
            for dr in range(1, n_row):
                landed(phead, ssem)


def pieces(x):
    hi = x.astype(jnp.bfloat16)
    rest = x - hi.astype(F32)
    mid = rest.astype(jnp.bfloat16)
    low = (rest - mid.astype(F32)).astype(jnp.bfloat16)
    return hi, mid, low


def update_kernel(rows, cols, tile, vwr, vwc, refl, coef, out, refl_out, coef_out, left, right, buf, sem, rsem):
    blocks = rows // LANES
    order = ((0, 0), (0, 1), (1, 0), (1, 1), (0, 2), (2, 0))
    two = 2 * K
    refl_copy = pltpu.make_async_copy(refl, refl_out, rsem)
    refl_copy.start()
    coef_out[...] = coef[:, 0:K]
    lp = pieces(vwr[...])
    wv = jnp.concatenate([vwc[K:two, :], vwc[0:K, :]], axis=0)
    rp = pieces(wv)
    for q, (a, b) in enumerate(order):
        left[q * two:(q + 1) * two, :] = lp[a]
        right[q * two:(q + 1) * two, :] = rp[b]

    def body(i, carry):
        part = pl.ds(pl.multiple_of(i * LANES, LANES), LANES)
        lt = left[:, part]
        change = lax.dot_general(lt, right[...], (((0,), (0,)), ((), ())), preferred_element_type=F32)
        buf[part, :] = tile[part, :] - change
        pltpu.make_async_copy(buf.at[part], out.at[part], sem).start()
        return carry

    lax.fori_loop(0, blocks, body, 0)
    pltpu.make_async_copy(buf, out, sem).wait()
    refl_copy.wait()


def make_per_device(n_row, n_col):
    def per_device(matrix):
        rows, cols = matrix.shape
        halves = cols // rows
        f32 = F32
        vmem = pl.BlockSpec(memory_space=pltpu.VMEM)
        anyspace = pl.BlockSpec(memory_space=pl.ANY)
        dma = pltpu.SemaphoreType.DMA
        full = n_row * rows
        rp = tile_rows(rows // LANES)

        def kernel(*refs):
            panel_kernel(rows, cols, n_row, n_col, *refs)

        def vm(*shape):
            return pltpu.VMEM(shape, f32)

        tile, refl, vwr, vwc, coef = pl.pallas_call(
            kernel,
            out_shape=(
                jax.ShapeDtypeStruct((rows, cols), f32),
                jax.ShapeDtypeStruct((K, full), f32),
                jax.ShapeDtypeStruct((2 * K, rows), f32),
                jax.ShapeDtypeStruct((2 * K, cols), f32),
                jax.ShapeDtypeStruct((2, LANES), f32),
            ),
            in_specs=[anyspace],
            out_specs=(vmem,) * 5,
            scratch_shapes=[
                vm(HEAD, cols), vm(HEAD, LANES), vm(K + 2, halves, rp, LANES), vm(K, n_col, halves, rp, LANES),
                vm(PAIRS, n_row, halves, rp, LANES), vm(PAIRS, n_col, rp, LANES),
                vm(PAIRS, n_row, 1, LANES), vm(PAIRS + 1, n_col, 1, LANES),
                vm(PAIRS, halves, rp, LANES), vm(PAIRS + 1, 3, rp, LANES),
                vm(PAIRS, 1, SUB, LANES), vm(PAIRS, 1, SUB, LANES),
                vm(2 * K, 1, rp, LANES), *[vm(1, rp, LANES)] * 5,
                vm(2 * K, halves, rp, LANES), *[vm(halves, rp, LANES)] * 5,
                vm(2 * K, 1, SUB, LANES), *[vm(1, SUB, LANES)] * 4,
                vm(2 * K, LANES), vm(2 * K, LANES), vm(2 * K, LANES), vm(8, LANES),
                vm(1, rp, LANES), vm(halves, rp, LANES), vm(rows, LANES), vm(rows, LANES),
                vm(2 * K + 2, SUB, LANES),
                dma((rows // LANES,)), dma, dma, dma((PAIRS + 1,)), dma((PAIRS,)),
                dma((PAIRS, halves)), dma((PAIRS,)), dma((PAIRS, halves)), dma((PAIRS,)),
                dma((PAIRS,)), dma((PAIRS + 1,)), dma((PAIRS + 1,)), dma((PAIRS,)),
                dma,
            ],
            compiler_params=pltpu.CompilerParams(
                collective_id=0, has_side_effects=True, vmem_limit_bytes=24 * 1024 * 1024),
        )(matrix)

        def update(*refs):
            update_kernel(rows, cols, *refs)

        return pl.pallas_call(
            update,
            out_shape=(
                jax.ShapeDtypeStruct((rows, cols), f32),
                jax.ShapeDtypeStruct((K, full), f32),
                jax.ShapeDtypeStruct((2, K), f32),
            ),
            in_specs=[vmem] * 5,
            out_specs=(anyspace, anyspace, vmem),
            scratch_shapes=[
                pltpu.VMEM((12 * K, rows), jnp.bfloat16),
                pltpu.VMEM((12 * K, cols), jnp.bfloat16),
                vm(rows, cols),
                dma, dma,
            ],
            compiler_params=pltpu.CompilerParams(vmem_limit_bytes=24 * 1024 * 1024),
        )(tile, vwr, vwc, refl, coef)
    return per_device


def solution(mesh):
    return jax.shard_map(
        make_per_device(mesh.shape["row"], mesh.shape["col"]),
        mesh=mesh,
        in_specs=(P("row", "col"),),
        out_specs=(P("row", "col"), P(), P()),
        check_vma=False,
    )
```

```python
import jax
import jax.numpy as jnp
from jax import lax
from jax.experimental import pallas as pl
from jax.experimental.pallas import tpu as pltpu
from jax.sharding import PartitionSpec as P

K = 16
PAIRS = K // 2
HEAD = 24
LANES = 128
SUB = 8
GROUPS = LANES // SUB
BATCH = 4
STEP = 3
MESH = pl.DeviceIdType.MESH
F32 = jnp.float32


def lanes_of(t):
    return slice(t * LANES, (t + 1) * LANES)


def tile_rows(n):
    return -(-n // SUB) * SUB


def spread_row(row):
    return jnp.broadcast_to(row, (LANES, LANES)).T


def panel_kernel(rows, cols, n_row, n_col, mat, tile, refl, vwr, vwc, coef,
                 headrows, phead, rowc, vout,
                 sum_a, sum_b, sc_a, sc_b, red_a, red_b, row_b, hd_a, hd_b,
                 wr, c0r, ur, pr, aur, qr, wc, c0c, uc, pc, auc, qc, wh, c0h, uh, ph, auh,
                 coefc, coefp, vuwu, scal, b0r, b0c, xs, accs, acca, dacc,
                 load_sem, hrow_sem, head_sem, row_sem, v_sem,
                 ya_sem, sa_sem, ra_sem, ha_sem, yb_sem, sb_sem, rb_sem, wb_sem, hb_sem,
                 ssem):
    halves = cols // rows
    r = lax.axis_index("row")
    c = lax.axis_index("col")
    blocks = rows // LANES
    ctiles = cols // LANES
    ut = rows // LANES // 2
    up = tile_rows(ut)
    ht = halves * ut
    diag = r // halves == c
    own_half = lax.rem(r, halves)

    def along_row(dr):
        return (lax.rem(r + dr, n_row), c)

    def along_col(dc):
        return (r, lax.rem(c + dc, n_col))

    def remote(src, dst, sem, device):
        return pltpu.make_async_remote_copy(src, dst, ssem, sem, device_id=device, device_id_type=MESH)

    def landed(ref, sem):
        pltpu.make_async_copy(ref, ref, sem).wait()

    def to_rows(ref, sem):
        for dr in range(1, n_row):
            remote(ref, ref, sem, along_row(dr)).start()

    def to_cols(ref, sem):
        for dc in range(1, n_col):
            remote(ref, ref, sem, along_col(dc)).start()

    def block_rows(k):
        return pl.ds(pl.multiple_of(k * LANES, LANES), LANES)

    def chunk(i):
        part = block_rows(i)
        return pltpu.make_async_copy(mat.at[part], tile.at[part], load_sem.at[i])

    hrow_copy = pltpu.make_async_copy(mat.at[0:HEAD], headrows, hrow_sem)
    pl.when(r == 0)(lambda: hrow_copy.start())

    def start_chunk(i, carry):
        chunk(i).start()
        return carry

    lax.fori_loop(0, blocks, start_chunk, 0)

    barrier = pltpu.get_barrier_semaphore()
    for dr in range(1, n_row):
        pl.semaphore_signal(barrier, inc=1, device_id=along_row(dr), device_id_type=MESH)
    for dc in range(1, n_col):
        pl.semaphore_signal(barrier, inc=1, device_id=along_col(dc), device_id_type=MESH)

    for ref in (wr, c0r, ur, pr, aur, wc, uc, pc, auc, wh, c0h, uh, ph, auh, coefc, coefp, vuwu, scal, coef, vwr, vwc):
        ref[...] = jnp.zeros_like(ref)
    if up > ut:
        for ref in (rowc, sum_a, sum_b, red_a, red_b, row_b):
            lead = ref.shape[:-2]
            ref[tuple(slice(None) for _ in lead) + (slice(ut, up),)] = jnp.zeros(lead + (up - ut, LANES), F32)

    def take_row(k):
        x = headrows[pl.ds(k, 1), :]
        for t in range(ctiles):
            rowc[k, t // ut, t % ut:t % ut + 1, :] = x[:, lanes_of(t)]

    @pl.when(r == 0)
    def _():
        hrow_copy.wait()
        take_row(0)
        take_row(1)

    pl.semaphore_wait(barrier, n_row + n_col - 2)

    @pl.when(r == 0)
    def _():
        to_rows(rowc.at[0:2, :, 0:ut], row_sem.at[0])

        @pl.when(c == 0)
        def _():
            phead[...] = headrows[:, 0:LANES]
            for dr in range(1, n_row):
                remote(headrows.at[:, 0:LANES], phead, head_sem, along_row(dr)).start()

    @pl.when(r != 0)
    def _():
        landed(rowc.at[0:2, :, 0:ut], row_sem.at[0])

    def positions(n, base):
        shape = (n, up, LANES)
        t = lax.broadcasted_iota(jnp.int32, shape, 1)
        x = (lax.broadcasted_iota(jnp.int32, shape, 0) * ut + t) * LANES + lax.broadcasted_iota(jnp.int32, shape, 2)
        return jnp.where(t < ut, x + base, -2)

    l128 = lax.broadcasted_iota(jnp.int32, (1, LANES), 1)
    pos_r = positions(2, r * rows)
    pos_c = positions(2 * halves, c * cols)
    pos_h = jnp.where(lax.broadcasted_iota(jnp.int32, (1, SUB, LANES), 1) < 1,
                      lax.broadcasted_iota(jnp.int32, (1, SUB, LANES), 2), -2)
    k16 = lax.broadcasted_iota(jnp.int32, (K, LANES), 0)
    s40 = lax.broadcasted_iota(jnp.int32, (2 * K + SUB, LANES), 0)
    t40 = lax.broadcasted_iota(jnp.int32, (2 * K + SUB, LANES), 1)
    eye40 = s40 == t40
    diag3 = (lax.broadcasted_iota(jnp.int32, (GROUPS, SUB, LANES), 0) * SUB
             + lax.broadcasted_iota(jnp.int32, (GROUPS, SUB, LANES), 1)
             == lax.broadcasted_iota(jnp.int32, (GROUPS, SUB, LANES), 2))

    def srow(k):
        return scal[k:k + 1, :]

    def splat(ref, k, like):
        return jnp.broadcast_to(ref[k:k + 1, :], like.shape[1:])[None]

    def weighted(w, ref, like, sl=slice(None)):
        acc = w[0, sl] * splat(ref, 0, like)
        for k in range(1, 2 * K):
            acc = acc + w[k, sl] * splat(ref, k, like)
        return acc

    def record(j, w, c0, u, p, au_ref, au, c0n, pn, pos, sl=slice(None)):
        kap, e, inv = splat(scal, 1, pos), splat(scal, 2, pos), splat(scal, 3, pos)
        hot = jnp.where(j >= 0, j + 1, -1)
        u_old = u[sl]
        un = jnp.where(pos > j + 1, (c0[sl] + e * u_old) * inv, 0.0)
        un = jnp.where(pos == hot, 1.0, un)
        fixed = p[sl] - kap * u_old
        w[K + j - 1, sl] = fixed
        w[jnp.maximum(j, 0), sl] = un
        w[K + j, sl] = pn
        c0[sl] = c0n
        u[sl] = un
        p[sl] = pn
        au_ref[sl] = au

    def advance(j, w, c0, u, p, au_ref, au, row, pos):
        ta = splat(scal, 0, pos) * au
        c0n = row - ta + weighted(w, coefc, pos)
        pn = ta - weighted(w, coefp, pos)
        record(j, w, c0, u, p, au_ref, au, c0n, pn, pos)

    def finish(j, h, w, c0, u, p, au_ref, q, total, row, row_next, pos, b0):
        n = pos.shape[0] // 2
        sl = slice(h * n, (h + 1) * n)
        ps = pos[sl]
        tau, kap, e, inv, uj1 = (splat(scal, k, pos) for k in (0, 1, 2, 3, 5))
        nxt = row_next[sl]
        aq = au_ref[sl] - row[sl] - uj1 * nxt
        au = (total + e * aq) * inv + nxt
        pn = tau * au - weighted(w, coefp, pos, sl)
        c0n = q[sl] + (2.0 * kap * uj1) * u[sl] - pn
        record(j, w, c0, u, p, au_ref, au, c0n, pn, ps, sl)
        b0[sl] = jnp.where(ps > j + 2, c0n, 0.0)

    def fold(x):
        y = x.reshape(-1, SUB, LANES)
        acc = y[0]
        for k in range(1, y.shape[0]):
            acc = acc + y[k]
        return acc

    def prepare(w, u, p, b0):
        x = b0[...]
        for k in range(2 * K):
            dacc[k] = fold(w[k] * x)
        dacc[2 * K] = fold(x * x)
        dacc[2 * K + 1] = fold(u[...] * p[...])

    def dots_row():
        acc = jnp.zeros((SUB, LANES), F32)
        for k in range(2 * K + 2):
            s = jnp.sum(dacc[k], axis=1, keepdims=True)
            acc = jnp.where(jnp.broadcast_to(l128, (SUB, LANES)) == k, s, acc)
        return jnp.sum(acc, axis=0, keepdims=True)

    def matvec_cols(i, mid):
        def reduce_block(k, base):
            a = accs[block_rows(k), :].reshape(GROUPS, SUB, LANES)
            s = jnp.sum(a, axis=2, keepdims=True)
            row = jnp.sum(jnp.sum(jnp.where(diag3, s, 0.0), axis=0), axis=0, keepdims=True)
            sum_b[i, c, base, pl.ds(k - base * ut, 1), :] = row

        def products(k, h, xb):
            for g in range(0, GROUPS, BATCH):
                piece = pl.ds(pl.multiple_of(k * LANES + g * SUB, SUB), BATCH * SUB)
                shape = (BATCH, SUB, LANES)
                acc = jnp.zeros(shape, F32) if h == 0 else accs[piece, :].reshape(shape)
                for t in range(ht):
                    acc = acc + tile[piece, lanes_of(h * ht + t)].reshape(shape) * xb[t][None]
                accs[piece, :] = acc.reshape(BATCH * SUB, LANES)

        def wide_x(h):
            ts = [h * ht + t for t in range(ht)]
            return [jnp.broadcast_to(b0c[t // ut, t % ut:t % ut + 1, :], (SUB, LANES)) for t in ts]

        xa = wide_x(0)

        def pass0(q, carry):
            for s in range(STEP):
                pl.when(i == 0)(lambda s=s: chunk(q * STEP + s).wait())
            for s in range(STEP):
                products(q * STEP + s, 0, xa)
            return carry

        lax.fori_loop(0, blocks // STEP, pass0, 0)
        mid()
        xb = wide_x(1)
        turns = ut // STEP
        for a in range(2):
            def pass1(q, carry, a=a, dots=False):
                if dots:
                    sc_b[i, c] = dots_row()
                for s in range(STEP):
                    products(q * STEP + s, 1, xb)
                    if s > 0:
                        reduce_block(q * STEP + s - 1, a)
                return carry

            for q in range(turns):
                early = a == 0 and q == 0
                pass1(a * turns + q, 0, a, early)
                if early:
                    to_cols(sc_b.at[i, c], sb_sem.at[i])
                reduce_block((a * turns + q) * STEP + STEP - 1, a)
            to_cols(sum_b.at[i, c, a, 0:ut], yb_sem.at[i, a])

    def spread(k, a):
        xs[block_rows(k), :] = spread_row(b0r[a, pl.ds(k - a * ut, 1), :])

    def spread_first(a):
        for s in range(STEP):
            spread(a * ut + s, a)

    def matvec_rows(i, mid):
        zero = jnp.zeros((SUB, LANES), F32)

        def products(k, acc, base):
            out = list(acc)
            for g in range(GROUPS):
                piece = pl.ds(pl.multiple_of(k * LANES + g * SUB, SUB), SUB)
                b = xs[piece, :]
                for t in range(len(out)):
                    out[t] = out[t] + tile[piece, lanes_of(base + t)] * b
            return tuple(out)

        def sweep(a, base, spreads):
            def body(q, acc):
                for s in range(STEP):
                    acc = products(q * STEP + s, acc, base)
                    if spreads and s == 0:
                        for n in range(STEP - 1):
                            spread(jnp.minimum((q + 1) * STEP + n, a * ut + ut - 1), a)
                    if spreads and s == 1:
                        spread(jnp.minimum((q + 1) * STEP + STEP - 1, a * ut + ut - 1), a)
                return acc
            return body

        turns = ut // STEP
        acc = lax.fori_loop(0, turns, sweep(0, 0, True), (zero,) * ctiles)
        for t in range(ctiles):
            acca[t] = acc[t]
        mid()
        for h in range(2):
            acc = tuple(acca[h * ht + t] for t in range(ht))
            acc = lax.fori_loop(turns, 2 * turns, sweep(1, h * ht, h == 0), acc)
            for t in range(ht):
                sum_a[i, r, h, t // ut, t % ut:t % ut + 1, :] = jnp.sum(acc[t], axis=0, keepdims=True)
            to_rows(sum_a.at[i, r, h, :, 0:ut], ya_sem.at[i, h])

    def head_advance(j, auh_row):
        advance(j, wh, c0h, uh, ph, auh, auh_row, phead[pl.ds(j + 1, 1), :][None] * jnp.ones((1, SUB, 1), F32), pos_h)

    def lane_pick(x, index):
        s = jnp.sum(jnp.where(l128 == index, x, 0.0), axis=1, keepdims=True)
        return jnp.broadcast_to(s, x.shape)

    def picks(j):
        head = wh[:, 0, 0, :]
        return (lane_pick(head, j), lane_pick(head, j + 1), lane_pick(c0h[0, 0:1, :], j + 1),
                lane_pick(uh[0, 0:1, :], j + 1), lane_pick(ph[0, 0:1, :], j))

    def pre_q(w, q, picked, row_next, pos):
        hj1 = picked[1]
        coefc[0:K, :] = hj1[K:2 * K]
        coefc[K:2 * K, :] = hj1[0:K]
        q[...] = row_next - weighted(w, coefc, pos)

    def scalars(j, sc, picked):
        hj, hj1, c0h1, uj1, pent = picked
        d = jnp.sum(jnp.where(eye40, jnp.broadcast_to(sc, eye40.shape), 0.0), axis=1, keepdims=True)
        d = jnp.broadcast_to(d, eye40.shape)
        vb, wb = d[0:K], d[K:2 * K]
        n0, kp = d[2 * K:2 * K + 1], d[2 * K + 1:2 * K + 2]
        hjv, hjw, hj1v, hj1w = hj[0:K], hj[K:2 * K], hj1[0:K], hj1[K:2 * K]
        last = k16 == j - 1
        tau_prev, bb_prev = srow(0), srow(4)
        kap = 0.5 * tau_prev * kp
        e = 2.0 * kap - pent
        lead = c0h1 + e * uj1
        n1 = jnp.sum(jnp.where(last, vb, 0.0), axis=0, keepdims=True)
        b2 = jnp.maximum(n0 + e * (2.0 * n1 + e * (bb_prev - uj1 * uj1)), 0.0)
        sig = jnp.sqrt(b2 + lead * lead)
        inv = 1.0 / (lead + sig)
        tau = 1.0 + lead / sig
        lk = jnp.where(last, kap, 0.0)
        hjw = hjw - lk * hjv
        hj1w = hj1w - lk * hj1v
        uu = bb_prev + 1.0
        vup = jnp.where(last, uu, vuwu[0:K, :])
        wup = jnp.where(last, kp - kap * uu, vuwu[K:2 * K, :])
        wb = wb - lk * vb
        vu = (vb + e * (vup - hjv - uj1 * hj1v)) * inv + hj1v
        wu = (wb + e * (wup - hjw - uj1 * hj1w)) * inv + hj1w
        beta = tau * vu - hj1v
        alpha = tau * wu - hj1w - lk * beta
        delta = tau * vu
        gamma = tau * wu - lk * delta
        coefc[0:K, :] = alpha
        coefc[K:2 * K, :] = beta
        coefp[0:K, :] = gamma
        coefp[K:2 * K, :] = delta
        vuwu[0:K, :] = vu
        vuwu[K:2 * K, :] = wu
        scal[0:1, :] = tau
        scal[1:2, :] = kap
        scal[2:3, :] = e
        scal[3:4, :] = inv
        scal[4:5, :] = b2 * inv * inv
        scal[5:6, :] = uj1
        coef[0:1, :] = jnp.where(l128 == j, tau, coef[0:1, :])
        coef[1:2, :] = jnp.where(l128 == j, -sig, coef[1:2, :])

    def slot_sum(read, n):
        acc = read(0)
        for s in range(1, n):
            acc = acc + read(s)
        return acc

    def flat(ref):
        n = ref.shape[0]
        return jnp.concatenate([ref[h, t:t + 1, :] for h in range(n) for t in range(ut)], axis=1)

    def send_v(k):
        vout[k, c] = wc[k]
        to_cols(vout.at[k, c, :, 0:ut], v_sem.at[k])

    def place_v(k):
        landed(vout.at[k, 0:n_col - 1, :, 0:ut], v_sem.at[k])
        refl[pl.ds(k, 1), :] = jnp.concatenate([flat(vout.at[k, s]) for s in range(n_col)], axis=1)

    def flat_v(k, w, out):
        out[pl.ds(k, 1), :] = flat(w.at[k])

    piece_c = pl.ds(own_half * 2, 2)

    def send_au_b(i):
        @pl.when(diag)
        def _():
            red_b[i] = auc[piece_c]
            to_cols(red_b.at[i, :, 0:ut], rb_sem.at[i])

    def send_rows_b(i):
        @pl.when(diag)
        def _():
            for q in range(2):
                row_b[i, q] = rowc[2 * i + q, piece_c]
            to_cols(row_b.at[i, :, :, 0:ut], wb_sem.at[i])

    def finish_cols(i, h):
        landed(sum_b.at[i, 0:n_col - 1, 0, 0:ut], yb_sem.at[i, h])
        finish(2 * i, h, wr, c0r, ur, pr, aur, qr, slot_sum(lambda s: sum_b[i, s, h:h + 1], n_col),
               row_b[i, 0], row_b[i, 1], pos_r, b0r)

    def finish_rows(i, h):
        landed(sum_a.at[i, 0:n_row - 1, 0, :, 0:ut], ya_sem.at[i, h])
        finish(2 * i + 1, h, wc, c0c, uc, pc, auc, qc, slot_sum(lambda s: sum_a[i, s, h], n_row),
               rowc[2 * i + 1], rowc[2 * i + 2], pos_c, b0c)

    def step_cols(i):
        j = 2 * i

        def mid():
            pl.when(i > 0)(lambda: finish_rows(jnp.maximum(i - 1, 0), 1))
            prepare(wc, uc, pc, b0c)
            send_au_b(i)

            @pl.when(c == 0)
            def _():
                hd_b[i] = auc[0:1, 0:SUB]
                to_cols(hd_b.at[i], hb_sem.at[i])

                @pl.when(i == 0)
                def _():
                    pl.when(r != 0)(lambda: landed(phead, head_sem))
                    to_cols(phead, head_sem)

        matvec_cols(i, mid)

        @pl.when(r == 0)
        def _():
            take_row(j + 2)
            take_row(j + 3)
            to_rows(rowc.at[pl.ds(j + 2, 2), :, 0:ut], row_sem.at[i + 1])

        @pl.when(jnp.logical_and(i == 0, c != 0))
        def _():
            landed(phead, head_sem)

        pl.when(jnp.logical_not(diag))(lambda: landed(row_b.at[i, :, :, 0:ut], wb_sem.at[i]))
        pl.when(c != 0)(lambda: landed(hd_b.at[i], hb_sem.at[i]))
        head_advance(j - 1, hd_b[i])
        picked = picks(j)
        pl.when(jnp.logical_not(diag))(lambda: landed(red_b.at[i, :, 0:ut], rb_sem.at[i]))
        advance(j - 1, wr, c0r, ur, pr, aur, red_b[i], row_b[i, 0], pos_r)
        pre_q(wr, qr, picked, row_b[i, 1], pos_r)
        landed(sc_b.at[i, 0:n_col - 1], sb_sem.at[i])
        scalars(j, slot_sum(lambda s: sc_b[i, s], n_col), picked)
        finish_cols(i, 0)
        spread_first(0)

    def step_rows(i):
        j = 2 * i + 1

        def mid():
            finish_cols(i, 1)
            spread_first(1)
            prepare(wr, ur, pr, b0r)
            sc_a[i, r] = dots_row()
            to_rows(sc_a.at[i, r], sa_sem.at[i])

            @pl.when(diag)
            def _():
                red_a[i, own_half] = aur[...]
                to_rows(red_a.at[i, own_half, :, 0:ut], ra_sem.at[i, own_half])

            @pl.when(r == 0)
            def _():
                hd_a[i] = aur[0:1, 0:SUB]
                to_rows(hd_a.at[i], ha_sem.at[i])

        matvec_rows(i, mid)

        pl.when(i > 0)(lambda: place_v(jnp.maximum(2 * i - 2, 0)))
        pl.when(i > 1)(lambda: place_v(jnp.maximum(2 * i - 3, 0)))
        pl.when(i > 0)(lambda: send_v(jnp.maximum(2 * i - 1, 0)))
        pl.when(r != 0)(lambda: landed(rowc.at[0:2, :, 0:ut], row_sem.at[i + 1]))
        send_rows_b(i + 1)
        pl.when(r != 0)(lambda: landed(hd_a.at[i], ha_sem.at[i]))
        head_advance(j - 1, hd_a[i])
        picked = picks(j)
        for h in range(halves):
            pl.when(r != halves * c + h)(lambda h=h: landed(red_a.at[i, h, :, 0:ut], ra_sem.at[i, h]))
        advance(j - 1, wc, c0c, uc, pc, auc, jnp.concatenate([red_a[i, h] for h in range(halves)], axis=0),
                rowc[j], pos_c)
        send_v(j - 1)
        pre_q(wc, qc, picked, rowc[j + 1], pos_c)
        landed(sc_a.at[i, 0:n_row - 1], sa_sem.at[i])
        scalars(j, slot_sum(lambda s: sc_a[i, s], n_row), picked)
        finish_rows(i, 0)

    def pair(i, carry):
        step_cols(i)
        step_rows(i)
        return carry

    c0c[...] = rowc[0]
    b0c[...] = jnp.where(pos_c > 1, rowc[0], 0.0)
    send_rows_b(0)
    lax.fori_loop(0, PAIRS, pair, 0)

    f = PAIRS
    finish_rows(f - 1, 1)
    send_au_b(f)
    kp = jnp.sum(fold(uc[...] * pc[...]), axis=1, keepdims=True)
    sc_b[f, c] = jnp.sum(jnp.broadcast_to(kp, (SUB, LANES)), axis=0, keepdims=True)
    to_cols(sc_b.at[f, c], sb_sem.at[f])
    send_v(K - 1)
    for k in range(2 * K - 1):
        flat_v(k, wc, vwc)
    for k in range(2 * K - 2):
        if k != K - 1:
            flat_v(k, wr, vwr)
    place_v(K - 3)
    place_v(K - 2)
    pl.when(jnp.logical_not(diag))(lambda: landed(row_b.at[f, :, :, 0:ut], wb_sem.at[f]))
    pl.when(jnp.logical_not(diag))(lambda: landed(red_b.at[f, :, 0:ut], rb_sem.at[f]))
    advance(K - 1, wr, c0r, ur, pr, aur, red_b[f], row_b[f, 0], pos_r)
    flat_v(K - 1, wr, vwr)
    flat_v(2 * K - 2, wr, vwr)
    landed(sc_b.at[f, 0:n_col - 1], sb_sem.at[f])
    kap = 0.5 * srow(0) * slot_sum(lambda s: sc_b[f, s], n_col)
    wr[2 * K - 1] = pr[...] - jnp.broadcast_to(kap, (up, LANES))[None] * ur[...]
    wc[2 * K - 1] = pc[...] - jnp.broadcast_to(kap, (up, LANES))[None] * uc[...]
    flat_v(2 * K - 1, wr, vwr)
    flat_v(2 * K - 1, wc, vwc)
    place_v(K - 1)

    def drain(i, carry):
        landed(sum_a.at[i, 0:n_row - 1, :, :, 0:ut], ssem)
        landed(sc_a.at[i, 0:n_row - 1], ssem)
        landed(sum_b.at[i, 0:n_col - 1, :, 0:ut], ssem)
        landed(sc_b.at[i, 0:n_col - 1], ssem)
        landed(vout.at[0:2, 0:n_col - 1, :, 0:ut], ssem)

        @pl.when(diag)
        def _():
            for dr in range(1, n_row):
                landed(red_a.at[i, 0, :, 0:ut], ssem)
            for dc in range(1, n_col):
                landed(red_b.at[i, :, 0:ut], ssem)
                landed(row_b.at[i, :, :, 0:ut], ssem)

        @pl.when(c == 0)
        def _():
            for dc in range(1, n_col):
                landed(hd_b.at[i], ssem)

        @pl.when(r == 0)
        def _():
            for dr in range(1, n_row):
                landed(hd_a.at[i], ssem)
                landed(rowc.at[0:2, :, 0:ut], ssem)
        return carry

    lax.fori_loop(0, PAIRS, drain, 0)
    landed(sc_b.at[f, 0:n_col - 1], ssem)

    @pl.when(diag)
    def _():
        for dc in range(1, n_col):
            landed(red_b.at[f, :, 0:ut], ssem)
            landed(row_b.at[f, :, :, 0:ut], ssem)

    @pl.when(r == 0)
    def _():
        for dr in range(1, n_row):
            landed(rowc.at[0:2, :, 0:ut], ssem)

    @pl.when(c == 0)
    def _():
        for dc in range(1, n_col):
            landed(phead, ssem)

        @pl.when(r == 0)
        def _():
            for dr in range(1, n_row):
                landed(phead, ssem)


def pieces(x):
    hi = x.astype(jnp.bfloat16)
    rest = x - hi.astype(F32)
    mid = rest.astype(jnp.bfloat16)
    low = (rest - mid.astype(F32)).astype(jnp.bfloat16)
    return hi, mid, low


def update_kernel(rows, cols, tile, vwr, vwc, refl, coef, out, refl_out, coef_out, left, right, buf, sem, rsem):
    blocks = rows // LANES
    order = ((0, 0), (0, 1), (1, 0), (1, 1), (0, 2), (2, 0))
    two = 2 * K
    refl_copy = pltpu.make_async_copy(refl, refl_out, rsem)
    refl_copy.start()
    coef_out[...] = coef[:, 0:K]
    lp = pieces(vwr[...])
    wv = jnp.concatenate([vwc[K:two, :], vwc[0:K, :]], axis=0)
    rp = pieces(wv)
    for q, (a, b) in enumerate(order):
        left[q * two:(q + 1) * two, :] = lp[a]
        right[q * two:(q + 1) * two, :] = rp[b]

    def body(i, carry):
        part = pl.ds(pl.multiple_of(i * LANES, LANES), LANES)
        lt = left[:, part]
        change = lax.dot_general(lt, right[...], (((0,), (0,)), ((), ())), preferred_element_type=F32)
        buf[part, :] = tile[part, :] - change
        pltpu.make_async_copy(buf.at[part], out.at[part], sem).start()
        return carry

    lax.fori_loop(0, blocks, body, 0)
    pltpu.make_async_copy(buf, out, sem).wait()
    refl_copy.wait()


def make_per_device(n_row, n_col):
    def per_device(matrix):
        rows, cols = matrix.shape
        halves = cols // rows
        f32 = F32
        vmem = pl.BlockSpec(memory_space=pltpu.VMEM)
        anyspace = pl.BlockSpec(memory_space=pl.ANY)
        dma = pltpu.SemaphoreType.DMA
        full = n_row * rows
        up = tile_rows(rows // LANES // 2)

        def kernel(*refs):
            panel_kernel(rows, cols, n_row, n_col, *refs)

        def vm(*shape):
            return pltpu.VMEM(shape, f32)

        tile, refl, vwr, vwc, coef = pl.pallas_call(
            kernel,
            out_shape=(
                jax.ShapeDtypeStruct((rows, cols), f32),
                jax.ShapeDtypeStruct((K, full), f32),
                jax.ShapeDtypeStruct((2 * K, rows), f32),
                jax.ShapeDtypeStruct((2 * K, cols), f32),
                jax.ShapeDtypeStruct((2, LANES), f32),
            ),
            in_specs=[anyspace],
            out_specs=(vmem,) * 5,
            scratch_shapes=[
                vm(HEAD, cols), vm(HEAD, LANES), vm(K + 2, 2 * halves, up, LANES),
                vm(K, n_col, 2 * halves, up, LANES),
                vm(PAIRS, n_row, 2, halves, up, LANES), vm(PAIRS, n_col, 2, up, LANES),
                vm(PAIRS, n_row, 1, LANES), vm(PAIRS + 1, n_col, 1, LANES),
                vm(PAIRS, halves, 2, up, LANES), vm(PAIRS + 1, 2, up, LANES), vm(PAIRS + 1, 2, 2, up, LANES),
                vm(PAIRS, 1, SUB, LANES), vm(PAIRS, 1, SUB, LANES),
                vm(2 * K, 2, up, LANES), *[vm(2, up, LANES)] * 5,
                vm(2 * K, 2 * halves, up, LANES), *[vm(2 * halves, up, LANES)] * 5,
                vm(2 * K, 1, SUB, LANES), *[vm(1, SUB, LANES)] * 4,
                vm(2 * K, LANES), vm(2 * K, LANES), vm(2 * K, LANES), vm(8, LANES),
                vm(2, up, LANES), vm(2 * halves, up, LANES), vm(rows, LANES), vm(rows, LANES),
                vm(cols // LANES, SUB, LANES), vm(2 * K + 2, SUB, LANES),
                dma((rows // LANES,)), dma, dma, dma((PAIRS + 1,)), dma((K,)),
                dma((PAIRS, 2)), dma((PAIRS,)), dma((PAIRS, halves)), dma((PAIRS,)),
                dma((PAIRS, 2)), dma((PAIRS + 1,)), dma((PAIRS + 1,)), dma((PAIRS + 1,)), dma((PAIRS,)),
                dma,
            ],
            compiler_params=pltpu.CompilerParams(
                collective_id=0, has_side_effects=True, vmem_limit_bytes=24 * 1024 * 1024),
        )(matrix)

        def update(*refs):
            update_kernel(rows, cols, *refs)

        return pl.pallas_call(
            update,
            out_shape=(
                jax.ShapeDtypeStruct((rows, cols), f32),
                jax.ShapeDtypeStruct((K, full), f32),
                jax.ShapeDtypeStruct((2, K), f32),
            ),
            in_specs=[vmem] * 5,
            out_specs=(anyspace, anyspace, vmem),
            scratch_shapes=[
                pltpu.VMEM((12 * K, rows), jnp.bfloat16),
                pltpu.VMEM((12 * K, cols), jnp.bfloat16),
                vm(rows, cols),
                dma, dma,
            ],
            compiler_params=pltpu.CompilerParams(vmem_limit_bytes=24 * 1024 * 1024),
        )(tile, vwr, vwc, refl, coef)
    return per_device


def solution(mesh):
    return jax.shard_map(
        make_per_device(mesh.shape["row"], mesh.shape["col"]),
        mesh=mesh,
        in_specs=(P("row", "col"),),
        out_specs=(P("row", "col"), P(), P()),
        check_vma=False,
    )
```

```python
import jax
import jax.numpy as jnp
from jax import lax
from jax.experimental import pallas as pl
from jax.experimental.pallas import tpu as pltpu
from jax.sharding import PartitionSpec as P

K = 16
PAIRS = K // 2
HEAD = 24
LANES = 128
SUB = 8
GROUPS = LANES // SUB
BATCH = 4
STEP = 3
MESH = pl.DeviceIdType.MESH
F32 = jnp.float32


def lanes_of(t):
    return slice(t * LANES, (t + 1) * LANES)


def tile_rows(n):
    return -(-n // SUB) * SUB


def spread_row(row):
    return jnp.broadcast_to(row, (LANES, LANES)).T


def panel_kernel(rows, cols, n_row, n_col, mat, tile, refl, vwr, vwc, coef,
                 headrows, phead, rowc, vout,
                 sum_a, sum_b, sc_a, sc_b, red_a, red_b, row_b, hd_a, hd_b,
                 wr, c0r, ur, pr, aur, qr, wc, c0c, uc, pc, auc, qc, wh, c0h, uh, ph, auh,
                 coefc, coefp, vuwu, scal, b0r, b0c, xs, accs, acca, dacc,
                 load_sem, hrow_sem, head_sem, row_sem, v_sem,
                 ya_sem, sa_sem, ra_sem, ha_sem, yb_sem, sb_sem, rb_sem, wb_sem, hb_sem,
                 ssem):
    halves = cols // rows
    r = lax.axis_index("row")
    c = lax.axis_index("col")
    blocks = rows // LANES
    ctiles = cols // LANES
    ut = rows // LANES // 2
    up = tile_rows(ut)
    ht = halves * ut
    diag = r // halves == c
    own_half = lax.rem(r, halves)

    def along_row(dr):
        return (lax.rem(r + dr, n_row), c)

    def along_col(dc):
        return (r, lax.rem(c + dc, n_col))

    def remote(src, dst, sem, device):
        return pltpu.make_async_remote_copy(src, dst, ssem, sem, device_id=device, device_id_type=MESH)

    def landed(ref, sem):
        pltpu.make_async_copy(ref, ref, sem).wait()

    def far_first(me, n):
        low = 2 * me < n
        out = []
        for t in range(n - 1):
            down = n - 1 - t
            out.append(jnp.where(low, jnp.where(down > me, down, down - 1), jnp.where(t < me, t, t + 1)))
        return out

    row_targets = far_first(r, n_row)
    col_targets = far_first(c, n_col)

    def to_rows(ref, sem):
        for t in row_targets:
            remote(ref, ref, sem, (t, c)).start()

    def to_cols(ref, sem):
        for t in col_targets:
            remote(ref, ref, sem, (r, t)).start()

    def block_rows(k):
        return pl.ds(pl.multiple_of(k * LANES, LANES), LANES)

    def chunk(i):
        part = block_rows(i)
        return pltpu.make_async_copy(mat.at[part], tile.at[part], load_sem.at[i])

    hrow_copy = pltpu.make_async_copy(mat.at[0:HEAD], headrows, hrow_sem)
    pl.when(r == 0)(lambda: hrow_copy.start())

    def start_chunk(i, carry):
        chunk(i).start()
        return carry

    lax.fori_loop(0, blocks, start_chunk, 0)

    barrier = pltpu.get_barrier_semaphore()
    for dr in range(1, n_row):
        pl.semaphore_signal(barrier, inc=1, device_id=along_row(dr), device_id_type=MESH)
    for dc in range(1, n_col):
        pl.semaphore_signal(barrier, inc=1, device_id=along_col(dc), device_id_type=MESH)

    for ref in (wr, c0r, ur, pr, aur, wc, uc, pc, auc, wh, c0h, uh, ph, auh, coefc, coefp, vuwu, scal, coef, vwr, vwc):
        ref[...] = jnp.zeros_like(ref)
    if up > ut:
        for ref in (rowc, sum_a, sum_b, red_a, red_b, row_b):
            lead = ref.shape[:-2]
            ref[tuple(slice(None) for _ in lead) + (slice(ut, up),)] = jnp.zeros(lead + (up - ut, LANES), F32)

    def take_row(k):
        x = headrows[pl.ds(k, 1), :]
        for t in range(ctiles):
            rowc[k, t // ut, t % ut:t % ut + 1, :] = x[:, lanes_of(t)]

    @pl.when(r == 0)
    def _():
        hrow_copy.wait()
        take_row(0)
        take_row(1)

    pl.semaphore_wait(barrier, n_row + n_col - 2)

    @pl.when(r == 0)
    def _():
        to_rows(rowc.at[0, 0:halves, 0:ut], row_sem.at[PAIRS + 1])
        to_rows(rowc.at[0, halves:2 * halves, 0:ut], row_sem.at[PAIRS + 2])
        to_rows(rowc.at[1, :, 0:ut], row_sem.at[0])

        @pl.when(c == 0)
        def _():
            phead[...] = headrows[:, 0:LANES]
            for dr in range(1, n_row):
                remote(headrows.at[:, 0:LANES], phead, head_sem, along_row(dr)).start()

    @pl.when(r != 0)
    def _():
        landed(rowc.at[0, 0:halves, 0:ut], row_sem.at[PAIRS + 1])

    def positions(n, base):
        shape = (n, up, LANES)
        t = lax.broadcasted_iota(jnp.int32, shape, 1)
        x = (lax.broadcasted_iota(jnp.int32, shape, 0) * ut + t) * LANES + lax.broadcasted_iota(jnp.int32, shape, 2)
        return jnp.where(t < ut, x + base, -2)

    l128 = lax.broadcasted_iota(jnp.int32, (1, LANES), 1)
    pos_r = positions(2, r * rows)
    pos_c = positions(2 * halves, c * cols)
    pos_h = jnp.where(lax.broadcasted_iota(jnp.int32, (1, SUB, LANES), 1) < 1,
                      lax.broadcasted_iota(jnp.int32, (1, SUB, LANES), 2), -2)
    k16 = lax.broadcasted_iota(jnp.int32, (K, LANES), 0)
    s40 = lax.broadcasted_iota(jnp.int32, (2 * K + SUB, LANES), 0)
    t40 = lax.broadcasted_iota(jnp.int32, (2 * K + SUB, LANES), 1)
    eye40 = s40 == t40
    diag3 = (lax.broadcasted_iota(jnp.int32, (GROUPS, SUB, LANES), 0) * SUB
             + lax.broadcasted_iota(jnp.int32, (GROUPS, SUB, LANES), 1)
             == lax.broadcasted_iota(jnp.int32, (GROUPS, SUB, LANES), 2))

    def srow(k):
        return scal[k:k + 1, :]

    def splat(ref, k, like):
        return jnp.broadcast_to(ref[k:k + 1, :], like.shape[1:])[None]

    def weighted(w, ref, like, sl=slice(None)):
        acc = w[0, sl] * splat(ref, 0, like)
        for k in range(1, 2 * K):
            acc = acc + w[k, sl] * splat(ref, k, like)
        return acc

    def record(j, w, c0, u, p, au_ref, au, c0n, pn, pos, sl=slice(None)):
        kap, e, inv = splat(scal, 1, pos), splat(scal, 2, pos), splat(scal, 3, pos)
        hot = jnp.where(j >= 0, j + 1, -1)
        u_old = u[sl]
        un = jnp.where(pos > j + 1, (c0[sl] + e * u_old) * inv, 0.0)
        un = jnp.where(pos == hot, 1.0, un)
        fixed = p[sl] - kap * u_old
        w[K + j - 1, sl] = fixed
        w[jnp.maximum(j, 0), sl] = un
        w[K + j, sl] = pn
        c0[sl] = c0n
        u[sl] = un
        p[sl] = pn
        au_ref[sl] = au

    def advance(j, w, c0, u, p, au_ref, au, row, pos):
        ta = splat(scal, 0, pos) * au
        c0n = row - ta + weighted(w, coefc, pos)
        pn = ta - weighted(w, coefp, pos)
        record(j, w, c0, u, p, au_ref, au, c0n, pn, pos)

    def finish(j, h, w, c0, u, p, au_ref, q, total, row, row_next, pos, b0):
        n = pos.shape[0] // 2
        sl = slice(h * n, (h + 1) * n)
        ps = pos[sl]
        tau, kap, e, inv, uj1 = (splat(scal, k, pos) for k in (0, 1, 2, 3, 5))
        nxt = row_next[sl]
        aq = au_ref[sl] - row[sl] - uj1 * nxt
        au = (total + e * aq) * inv + nxt
        pn = tau * au - weighted(w, coefp, pos, sl)
        c0n = q[sl] + (2.0 * kap * uj1) * u[sl] - pn
        record(j, w, c0, u, p, au_ref, au, c0n, pn, ps, sl)
        b0[sl] = jnp.where(ps > j + 2, c0n, 0.0)

    def fold(x):
        y = x.reshape(-1, SUB, LANES)
        acc = y[0]
        for k in range(1, y.shape[0]):
            acc = acc + y[k]
        return acc

    def prepare(w, u, p, b0):
        x = b0[...]
        for k in range(2 * K):
            dacc[k] = fold(w[k] * x)
        dacc[2 * K] = fold(x * x)
        dacc[2 * K + 1] = fold(u[...] * p[...])

    def dots_row():
        acc = jnp.zeros((SUB, LANES), F32)
        for k in range(2 * K + 2):
            s = jnp.sum(dacc[k], axis=1, keepdims=True)
            acc = jnp.where(jnp.broadcast_to(l128, (SUB, LANES)) == k, s, acc)
        return jnp.sum(acc, axis=0, keepdims=True)

    def matvec_cols(i, mid):
        def reduce_block(k, base):
            a = accs[block_rows(k), :].reshape(GROUPS, SUB, LANES)
            s = jnp.sum(a, axis=2, keepdims=True)
            row = jnp.sum(jnp.sum(jnp.where(diag3, s, 0.0), axis=0), axis=0, keepdims=True)
            sum_b[i, c, base, pl.ds(k - base * ut, 1), :] = row

        def products(k, h, xb):
            for g in range(0, GROUPS, BATCH):
                piece = pl.ds(pl.multiple_of(k * LANES + g * SUB, SUB), BATCH * SUB)
                shape = (BATCH, SUB, LANES)
                acc = jnp.zeros(shape, F32) if h == 0 else accs[piece, :].reshape(shape)
                for t in range(ht):
                    acc = acc + tile[piece, lanes_of(h * ht + t)].reshape(shape) * xb[t][None]
                accs[piece, :] = acc.reshape(BATCH * SUB, LANES)

        def wide_x(h):
            ts = [h * ht + t for t in range(ht)]
            return [jnp.broadcast_to(b0c[t // ut, t % ut:t % ut + 1, :], (SUB, LANES)) for t in ts]

        xa = wide_x(0)

        def pass0(q, carry):
            for s in range(STEP):
                pl.when(i == 0)(lambda s=s: chunk(q * STEP + s).wait())
            for s in range(STEP):
                products(q * STEP + s, 0, xa)
            return carry

        lax.fori_loop(0, blocks // STEP, pass0, 0)
        mid()
        xb = wide_x(1)
        turns = ut // STEP
        for a in range(2):
            def pass1(q, carry, a=a, dots=False):
                if dots:
                    sc_b[i, c] = dots_row()
                for s in range(STEP):
                    products(q * STEP + s, 1, xb)
                    if s > 0:
                        reduce_block(q * STEP + s - 1, a)
                return carry

            for q in range(turns):
                early = a == 0 and q == 0
                pass1(a * turns + q, 0, a, early)
                if early:
                    to_cols(sc_b.at[i, c], sb_sem.at[i])
                reduce_block((a * turns + q) * STEP + STEP - 1, a)
            to_cols(sum_b.at[i, c, a, 0:ut], yb_sem.at[i, a])

    def spread(k, a):
        xs[block_rows(k), :] = spread_row(b0r[a, pl.ds(k - a * ut, 1), :])

    def spread_first(a):
        for s in range(STEP):
            spread(a * ut + s, a)

    def matvec_rows(i, mid):
        zero = jnp.zeros((SUB, LANES), F32)

        def products(k, acc, base):
            out = list(acc)
            for g in range(GROUPS):
                piece = pl.ds(pl.multiple_of(k * LANES + g * SUB, SUB), SUB)
                b = xs[piece, :]
                for t in range(len(out)):
                    out[t] = out[t] + tile[piece, lanes_of(base + t)] * b
            return tuple(out)

        def ahead(k, a):
            spread(jnp.minimum(k, a * ut + ut - 1), a)

        def sweep(a, base, lead, dots=False):
            def body(q, acc):
                if dots:
                    sc_a[i, r] = dots_row()
                for s in range(STEP):
                    acc = products(q * STEP + s, acc, base)
                    if lead and s == 0:
                        for n in range(STEP - 1):
                            ahead(q * STEP + lead + n, a)
                    if lead and s == 1:
                        ahead(q * STEP + lead + STEP - 1, a)
                return acc
            return body

        turns = ut // STEP
        acc = lax.fori_loop(0, turns, sweep(0, 0, 1), (zero,) * ctiles)
        for t in range(ctiles):
            acca[t] = acc[t]
        mid()
        for h in range(2):
            acc = tuple(acca[h * ht + t] for t in range(ht))
            lead = STEP if h == 0 else 0
            if h == 0:
                cut = turns + jnp.minimum(i + 1, 1)
                acc = lax.fori_loop(turns, cut, sweep(1, 0, lead, True), acc)
                to_rows(sc_a.at[i, r], sa_sem.at[i])
                acc = lax.fori_loop(cut, 2 * turns, sweep(1, 0, lead), acc)
            else:
                acc = lax.fori_loop(turns, 2 * turns, sweep(1, h * ht, 0), acc)
            for t in range(ht):
                sum_a[i, r, h, t // ut, t % ut:t % ut + 1, :] = jnp.sum(acc[t], axis=0, keepdims=True)
            to_rows(sum_a.at[i, r, h, :, 0:ut], ya_sem.at[i, h])

    def head_advance(j, auh_row):
        advance(j, wh, c0h, uh, ph, auh, auh_row, phead[pl.ds(j + 1, 1), :][None] * jnp.ones((1, SUB, 1), F32), pos_h)

    def lane_pick(x, index):
        s = jnp.sum(jnp.where(l128 == index, x, 0.0), axis=1, keepdims=True)
        return jnp.broadcast_to(s, x.shape)

    def picks(j):
        head = wh[:, 0, 0, :]
        return (lane_pick(head, j), lane_pick(head, j + 1), lane_pick(c0h[0, 0:1, :], j + 1),
                lane_pick(uh[0, 0:1, :], j + 1), lane_pick(ph[0, 0:1, :], j))

    def pre_q(w, q, picked, row_next, pos):
        hj1 = picked[1]
        coefc[0:K, :] = hj1[K:2 * K]
        coefc[K:2 * K, :] = hj1[0:K]
        q[...] = row_next - weighted(w, coefc, pos)

    def scalars(j, sc, picked):
        hj, hj1, c0h1, uj1, pent = picked
        d = jnp.sum(jnp.where(eye40, jnp.broadcast_to(sc, eye40.shape), 0.0), axis=1, keepdims=True)
        d = jnp.broadcast_to(d, eye40.shape)
        vb, wb = d[0:K], d[K:2 * K]
        n0, kp = d[2 * K:2 * K + 1], d[2 * K + 1:2 * K + 2]
        hjv, hjw, hj1v, hj1w = hj[0:K], hj[K:2 * K], hj1[0:K], hj1[K:2 * K]
        last = k16 == j - 1
        tau_prev, bb_prev = srow(0), srow(4)
        kap = 0.5 * tau_prev * kp
        e = 2.0 * kap - pent
        lead = c0h1 + e * uj1
        n1 = jnp.sum(jnp.where(last, vb, 0.0), axis=0, keepdims=True)
        b2 = jnp.maximum(n0 + e * (2.0 * n1 + e * (bb_prev - uj1 * uj1)), 0.0)
        sig = jnp.sqrt(b2 + lead * lead)
        inv = 1.0 / (lead + sig)
        tau = 1.0 + lead / sig
        lk = jnp.where(last, kap, 0.0)
        hjw = hjw - lk * hjv
        hj1w = hj1w - lk * hj1v
        uu = bb_prev + 1.0
        vup = jnp.where(last, uu, vuwu[0:K, :])
        wup = jnp.where(last, kp - kap * uu, vuwu[K:2 * K, :])
        wb = wb - lk * vb
        vu = (vb + e * (vup - hjv - uj1 * hj1v)) * inv + hj1v
        wu = (wb + e * (wup - hjw - uj1 * hj1w)) * inv + hj1w
        beta = tau * vu - hj1v
        alpha = tau * wu - hj1w - lk * beta
        delta = tau * vu
        gamma = tau * wu - lk * delta
        coefc[0:K, :] = alpha
        coefc[K:2 * K, :] = beta
        coefp[0:K, :] = gamma
        coefp[K:2 * K, :] = delta
        vuwu[0:K, :] = vu
        vuwu[K:2 * K, :] = wu
        scal[0:1, :] = tau
        scal[1:2, :] = kap
        scal[2:3, :] = e
        scal[3:4, :] = inv
        scal[4:5, :] = b2 * inv * inv
        scal[5:6, :] = uj1
        coef[0:1, :] = jnp.where(l128 == j, tau, coef[0:1, :])
        coef[1:2, :] = jnp.where(l128 == j, -sig, coef[1:2, :])

    def slot_sum(read, n):
        acc = read(0)
        for s in range(1, n):
            acc = acc + read(s)
        return acc

    def flat(ref):
        n = ref.shape[0]
        return jnp.concatenate([ref[h, t:t + 1, :] for h in range(n) for t in range(ut)], axis=1)

    def send_v(k):
        vout[k, c] = wc[k]
        to_cols(vout.at[k, c, :, 0:ut], v_sem.at[k])

    def place_v(k):
        landed(vout.at[k, 0:n_col - 1, :, 0:ut], v_sem.at[k])
        refl[pl.ds(k, 1), :] = jnp.concatenate([flat(vout.at[k, s]) for s in range(n_col)], axis=1)

    def flat_v(k, w, out):
        out[pl.ds(k, 1), :] = flat(w.at[k])

    piece_c = pl.ds(own_half * 2, 2)

    def send_au_b(i):
        @pl.when(diag)
        def _():
            red_b[i] = auc[piece_c]
            to_cols(red_b.at[i, :, 0:ut], rb_sem.at[i])

    def send_rows_b(i):
        @pl.when(diag)
        def _():
            for q in range(2):
                row_b[i, q] = rowc[2 * i + q, piece_c]
            to_cols(row_b.at[i, :, :, 0:ut], wb_sem.at[i])

    def finish_cols(i, h):
        landed(sum_b.at[i, 0:n_col - 1, 0, 0:ut], yb_sem.at[i, h])
        finish(2 * i, h, wr, c0r, ur, pr, aur, qr, slot_sum(lambda s: sum_b[i, s, h:h + 1], n_col),
               row_b[i, 0], row_b[i, 1], pos_r, b0r)

    def finish_rows(i, h):
        landed(sum_a.at[i, 0:n_row - 1, 0, :, 0:ut], ya_sem.at[i, h])
        finish(2 * i + 1, h, wc, c0c, uc, pc, auc, qc, slot_sum(lambda s: sum_a[i, s, h], n_row),
               rowc[2 * i + 1], rowc[2 * i + 2], pos_c, b0c)

    def start_half(h):
        sl = slice(h * halves, (h + 1) * halves)
        x = rowc[0, sl]
        c0c[sl] = x
        b0c[sl] = jnp.where(pos_c[sl] > 1, x, 0.0)

    def step_cols(i):
        j = 2 * i

        def mid():
            @pl.when(i == 0)
            def _():
                @pl.when(r != 0)
                def _():
                    landed(rowc.at[0, 0:halves, 0:ut], row_sem.at[PAIRS + 2])
                    landed(rowc.at[1, :, 0:ut], row_sem.at[0])

                start_half(1)
                send_rows_b(0)

            pl.when(i > 0)(lambda: finish_rows(jnp.maximum(i - 1, 0), 1))
            prepare(wc, uc, pc, b0c)
            send_au_b(i)

            @pl.when(c == 0)
            def _():
                hd_b[i] = auc[0:1, 0:SUB]
                to_cols(hd_b.at[i], hb_sem.at[i])

                @pl.when(i == 0)
                def _():
                    pl.when(r != 0)(lambda: landed(phead, head_sem))
                    to_cols(phead, head_sem)

        matvec_cols(i, mid)

        @pl.when(r == 0)
        def _():
            take_row(j + 2)
            take_row(j + 3)
            to_rows(rowc.at[pl.ds(j + 2, 2), :, 0:ut], row_sem.at[i + 1])

        @pl.when(jnp.logical_and(i == 0, c != 0))
        def _():
            landed(phead, head_sem)

        pl.when(jnp.logical_not(diag))(lambda: landed(row_b.at[i, :, :, 0:ut], wb_sem.at[i]))
        pl.when(c != 0)(lambda: landed(hd_b.at[i], hb_sem.at[i]))
        head_advance(j - 1, hd_b[i])
        picked = picks(j)
        pl.when(jnp.logical_not(diag))(lambda: landed(red_b.at[i, :, 0:ut], rb_sem.at[i]))
        advance(j - 1, wr, c0r, ur, pr, aur, red_b[i], row_b[i, 0], pos_r)
        pre_q(wr, qr, picked, row_b[i, 1], pos_r)
        landed(sc_b.at[i, 0:n_col - 1], sb_sem.at[i])
        scalars(j, slot_sum(lambda s: sc_b[i, s], n_col), picked)
        finish_cols(i, 0)
        spread(0, 0)

    def step_rows(i):
        j = 2 * i + 1

        def mid():
            finish_cols(i, 1)
            spread_first(1)
            prepare(wr, ur, pr, b0r)

            @pl.when(diag)
            def _():
                red_a[i, own_half] = aur[...]
                to_rows(red_a.at[i, own_half, :, 0:ut], ra_sem.at[i, own_half])

            @pl.when(r == 0)
            def _():
                hd_a[i] = aur[0:1, 0:SUB]
                to_rows(hd_a.at[i], ha_sem.at[i])

        matvec_rows(i, mid)

        pl.when(i > 0)(lambda: place_v(jnp.maximum(2 * i - 2, 0)))
        pl.when(i > 1)(lambda: place_v(jnp.maximum(2 * i - 3, 0)))
        pl.when(i > 0)(lambda: send_v(jnp.maximum(2 * i - 1, 0)))
        pl.when(r != 0)(lambda: landed(rowc.at[0:2, :, 0:ut], row_sem.at[i + 1]))
        send_rows_b(i + 1)
        pl.when(r != 0)(lambda: landed(hd_a.at[i], ha_sem.at[i]))
        head_advance(j - 1, hd_a[i])
        picked = picks(j)
        for h in range(halves):
            pl.when(r != halves * c + h)(lambda h=h: landed(red_a.at[i, h, :, 0:ut], ra_sem.at[i, h]))
        advance(j - 1, wc, c0c, uc, pc, auc, jnp.concatenate([red_a[i, h] for h in range(halves)], axis=0),
                rowc[j], pos_c)
        send_v(j - 1)
        pre_q(wc, qc, picked, rowc[j + 1], pos_c)
        landed(sc_a.at[i, 0:n_row - 1], sa_sem.at[i])
        scalars(j, slot_sum(lambda s: sc_a[i, s], n_row), picked)
        finish_rows(i, 0)

    def pair(i, carry):
        step_cols(i)
        step_rows(i)
        return carry

    start_half(0)
    lax.fori_loop(0, PAIRS, pair, 0)

    f = PAIRS
    finish_rows(f - 1, 1)
    send_au_b(f)
    kp = jnp.sum(fold(uc[...] * pc[...]), axis=1, keepdims=True)
    sc_b[f, c] = jnp.sum(jnp.broadcast_to(kp, (SUB, LANES)), axis=0, keepdims=True)
    to_cols(sc_b.at[f, c], sb_sem.at[f])
    send_v(K - 1)
    for k in range(2 * K - 1):
        flat_v(k, wc, vwc)
    for k in range(2 * K - 2):
        if k != K - 1:
            flat_v(k, wr, vwr)
    place_v(K - 3)
    place_v(K - 2)
    pl.when(jnp.logical_not(diag))(lambda: landed(row_b.at[f, :, :, 0:ut], wb_sem.at[f]))
    pl.when(jnp.logical_not(diag))(lambda: landed(red_b.at[f, :, 0:ut], rb_sem.at[f]))
    advance(K - 1, wr, c0r, ur, pr, aur, red_b[f], row_b[f, 0], pos_r)
    flat_v(K - 1, wr, vwr)
    flat_v(2 * K - 2, wr, vwr)
    landed(sc_b.at[f, 0:n_col - 1], sb_sem.at[f])
    kap = 0.5 * srow(0) * slot_sum(lambda s: sc_b[f, s], n_col)
    wr[2 * K - 1] = pr[...] - jnp.broadcast_to(kap, (up, LANES))[None] * ur[...]
    wc[2 * K - 1] = pc[...] - jnp.broadcast_to(kap, (up, LANES))[None] * uc[...]
    flat_v(2 * K - 1, wr, vwr)
    flat_v(2 * K - 1, wc, vwc)
    place_v(K - 1)

    def drain(i, carry):
        landed(sum_a.at[i, 0:n_row - 1, :, :, 0:ut], ssem)
        landed(sc_a.at[i, 0:n_row - 1], ssem)
        landed(sum_b.at[i, 0:n_col - 1, :, 0:ut], ssem)
        landed(sc_b.at[i, 0:n_col - 1], ssem)
        landed(vout.at[0:2, 0:n_col - 1, :, 0:ut], ssem)

        @pl.when(diag)
        def _():
            for dr in range(1, n_row):
                landed(red_a.at[i, 0, :, 0:ut], ssem)
            for dc in range(1, n_col):
                landed(red_b.at[i, :, 0:ut], ssem)
                landed(row_b.at[i, :, :, 0:ut], ssem)

        @pl.when(c == 0)
        def _():
            for dc in range(1, n_col):
                landed(hd_b.at[i], ssem)

        @pl.when(r == 0)
        def _():
            for dr in range(1, n_row):
                landed(hd_a.at[i], ssem)
                landed(rowc.at[0:2, :, 0:ut], ssem)
        return carry

    lax.fori_loop(0, PAIRS, drain, 0)
    landed(sc_b.at[f, 0:n_col - 1], ssem)

    @pl.when(diag)
    def _():
        for dc in range(1, n_col):
            landed(red_b.at[f, :, 0:ut], ssem)
            landed(row_b.at[f, :, :, 0:ut], ssem)

    @pl.when(r == 0)
    def _():
        for dr in range(1, n_row):
            landed(rowc.at[0:2, :, 0:ut], ssem)

    @pl.when(c == 0)
    def _():
        for dc in range(1, n_col):
            landed(phead, ssem)

        @pl.when(r == 0)
        def _():
            for dr in range(1, n_row):
                landed(phead, ssem)


def pieces(x):
    hi = x.astype(jnp.bfloat16)
    rest = x - hi.astype(F32)
    mid = rest.astype(jnp.bfloat16)
    low = (rest - mid.astype(F32)).astype(jnp.bfloat16)
    return hi, mid, low


def update_kernel(rows, cols, tile, vwr, vwc, refl, coef, out, refl_out, coef_out, left, right, buf, sem, rsem):
    blocks = rows // LANES
    order = ((0, 0), (0, 1), (1, 0), (1, 1), (0, 2), (2, 0))
    two = 2 * K
    refl_copy = pltpu.make_async_copy(refl, refl_out, rsem)
    refl_copy.start()
    coef_out[...] = coef[:, 0:K]
    lp = pieces(vwr[...])
    wv = jnp.concatenate([vwc[K:two, :], vwc[0:K, :]], axis=0)
    rp = pieces(wv)
    for q, (a, b) in enumerate(order):
        left[q * two:(q + 1) * two, :] = lp[a]
        right[q * two:(q + 1) * two, :] = rp[b]

    def body(i, carry):
        part = pl.ds(pl.multiple_of(i * LANES, LANES), LANES)
        lt = left[:, part]
        change = lax.dot_general(lt, right[...], (((0,), (0,)), ((), ())), preferred_element_type=F32)
        buf[part, :] = tile[part, :] - change
        pltpu.make_async_copy(buf.at[part], out.at[part], sem).start()
        return carry

    lax.fori_loop(0, blocks, body, 0)
    pltpu.make_async_copy(buf, out, sem).wait()
    refl_copy.wait()


def make_per_device(n_row, n_col):
    def per_device(matrix):
        rows, cols = matrix.shape
        halves = cols // rows
        f32 = F32
        vmem = pl.BlockSpec(memory_space=pltpu.VMEM)
        anyspace = pl.BlockSpec(memory_space=pl.ANY)
        dma = pltpu.SemaphoreType.DMA
        full = n_row * rows
        up = tile_rows(rows // LANES // 2)

        def kernel(*refs):
            panel_kernel(rows, cols, n_row, n_col, *refs)

        def vm(*shape):
            return pltpu.VMEM(shape, f32)

        tile, refl, vwr, vwc, coef = pl.pallas_call(
            kernel,
            out_shape=(
                jax.ShapeDtypeStruct((rows, cols), f32),
                jax.ShapeDtypeStruct((K, full), f32),
                jax.ShapeDtypeStruct((2 * K, rows), f32),
                jax.ShapeDtypeStruct((2 * K, cols), f32),
                jax.ShapeDtypeStruct((2, LANES), f32),
            ),
            in_specs=[anyspace],
            out_specs=(vmem,) * 5,
            scratch_shapes=[
                vm(HEAD, cols), vm(HEAD, LANES), vm(K + 2, 2 * halves, up, LANES),
                vm(K, n_col, 2 * halves, up, LANES),
                vm(PAIRS, n_row, 2, halves, up, LANES), vm(PAIRS, n_col, 2, up, LANES),
                vm(PAIRS, n_row, 1, LANES), vm(PAIRS + 1, n_col, 1, LANES),
                vm(PAIRS, halves, 2, up, LANES), vm(PAIRS + 1, 2, up, LANES), vm(PAIRS + 1, 2, 2, up, LANES),
                vm(PAIRS, 1, SUB, LANES), vm(PAIRS, 1, SUB, LANES),
                vm(2 * K, 2, up, LANES), *[vm(2, up, LANES)] * 5,
                vm(2 * K, 2 * halves, up, LANES), *[vm(2 * halves, up, LANES)] * 5,
                vm(2 * K, 1, SUB, LANES), *[vm(1, SUB, LANES)] * 4,
                vm(2 * K, LANES), vm(2 * K, LANES), vm(2 * K, LANES), vm(8, LANES),
                vm(2, up, LANES), vm(2 * halves, up, LANES), vm(rows, LANES), vm(rows, LANES),
                vm(cols // LANES, SUB, LANES), vm(2 * K + 2, SUB, LANES),
                dma((rows // LANES,)), dma, dma, dma((PAIRS + 3,)), dma((K,)),
                dma((PAIRS, 2)), dma((PAIRS,)), dma((PAIRS, halves)), dma((PAIRS,)),
                dma((PAIRS, 2)), dma((PAIRS + 1,)), dma((PAIRS + 1,)), dma((PAIRS + 1,)), dma((PAIRS,)),
                dma,
            ],
            compiler_params=pltpu.CompilerParams(
                collective_id=0, has_side_effects=True, vmem_limit_bytes=24 * 1024 * 1024),
        )(matrix)

        def update(*refs):
            update_kernel(rows, cols, *refs)

        return pl.pallas_call(
            update,
            out_shape=(
                jax.ShapeDtypeStruct((rows, cols), f32),
                jax.ShapeDtypeStruct((K, full), f32),
                jax.ShapeDtypeStruct((2, K), f32),
            ),
            in_specs=[vmem] * 5,
            out_specs=(anyspace, anyspace, vmem),
            scratch_shapes=[
                pltpu.VMEM((12 * K, rows), jnp.bfloat16),
                pltpu.VMEM((12 * K, cols), jnp.bfloat16),
                vm(rows, cols),
                dma, dma,
            ],
            compiler_params=pltpu.CompilerParams(vmem_limit_bytes=24 * 1024 * 1024),
        )(tile, vwr, vwc, refl, coef)
    return per_device


def solution(mesh):
    return jax.shard_map(
        make_per_device(mesh.shape["row"], mesh.shape["col"]),
        mesh=mesh,
        in_specs=(P("row", "col"),),
        out_specs=(P("row", "col"), P(), P()),
        check_vma=False,
    )
```

```python
import jax
import jax.numpy as jnp
from jax import lax
from jax.experimental import pallas as pl
from jax.experimental.pallas import tpu as pltpu
from jax.sharding import PartitionSpec as P

K = 16
PAIRS = K // 2
HEAD = 24
LANES = 128
SUB = 8
GROUPS = LANES // SUB
BATCH = 8
STEP = 3
MESH = pl.DeviceIdType.MESH
F32 = jnp.float32


def lanes_of(t):
    return slice(t * LANES, (t + 1) * LANES)


def tile_rows(n):
    return -(-n // SUB) * SUB


def spread_row(row):
    return jnp.broadcast_to(row, (LANES, LANES)).T


def panel_kernel(rows, cols, n_row, n_col, mat, tile, refl, vwr, vwc, coef,
                 headrows, phead, rowc, vout,
                 sum_a, sum_b, sc_a, sc_b, red_a, red_b, row_b, hd_a, hd_b,
                 wr, c0r, ur, pr, aur, qr, wc, c0c, uc, pc, auc, qc, wh, c0h, uh, ph, auh,
                 coefc, coefp, vuwu, scal, b0r, b0c, xs, accs, acca, dacc,
                 load_sem, hrow_sem, head_sem, row_sem, v_sem,
                 ya_sem, sa_sem, ra_sem, ha_sem, yb_sem, sb_sem, rb_sem, wb_sem, hb_sem,
                 ssem):
    halves = cols // rows
    r = lax.axis_index("row")
    c = lax.axis_index("col")
    blocks = rows // LANES
    ctiles = cols // LANES
    ut = rows // LANES // 2
    up = tile_rows(ut)
    ht = halves * ut
    diag = r // halves == c
    own_half = lax.rem(r, halves)

    def along_row(dr):
        return (lax.rem(r + dr, n_row), c)

    def along_col(dc):
        return (r, lax.rem(c + dc, n_col))

    def remote(src, dst, sem, device):
        return pltpu.make_async_remote_copy(src, dst, ssem, sem, device_id=device, device_id_type=MESH)

    def landed(ref, sem):
        pltpu.make_async_copy(ref, ref, sem).wait()

    def far_first(me, n):
        low = 2 * me < n
        out = []
        for t in range(n - 1):
            down = n - 1 - t
            out.append(jnp.where(low, jnp.where(down > me, down, down - 1), jnp.where(t < me, t, t + 1)))
        return out

    row_targets = far_first(r, n_row)
    col_targets = far_first(c, n_col)

    def to_rows(ref, sem):
        for t in row_targets:
            remote(ref, ref, sem, (t, c)).start()

    def to_cols(ref, sem):
        for t in col_targets:
            remote(ref, ref, sem, (r, t)).start()

    def block_rows(k):
        return pl.ds(pl.multiple_of(k * LANES, LANES), LANES)

    def chunk(i):
        part = block_rows(i)
        return pltpu.make_async_copy(mat.at[part], tile.at[part], load_sem.at[i])

    hrow_copy = pltpu.make_async_copy(mat.at[0:HEAD], headrows, hrow_sem)
    pl.when(r == 0)(lambda: hrow_copy.start())

    def start_chunk(i, carry):
        chunk(i).start()
        return carry

    lax.fori_loop(0, blocks, start_chunk, 0)

    barrier = pltpu.get_barrier_semaphore()
    for dr in range(1, n_row):
        pl.semaphore_signal(barrier, inc=1, device_id=along_row(dr), device_id_type=MESH)
    for dc in range(1, n_col):
        pl.semaphore_signal(barrier, inc=1, device_id=along_col(dc), device_id_type=MESH)

    for ref in (wr, c0r, ur, pr, aur, wc, uc, pc, auc, wh, c0h, uh, ph, auh, coefc, coefp, vuwu, scal, coef, vwr, vwc):
        ref[...] = jnp.zeros_like(ref)
    if up > ut:
        for ref in (rowc, sum_a, sum_b, red_a, red_b, row_b):
            lead = ref.shape[:-2]
            ref[tuple(slice(None) for _ in lead) + (slice(ut, up),)] = jnp.zeros(lead + (up - ut, LANES), F32)

    def take_row(k):
        x = headrows[pl.ds(k, 1), :]
        for t in range(ctiles):
            rowc[k, t // ut, t % ut:t % ut + 1, :] = x[:, lanes_of(t)]

    @pl.when(r == 0)
    def _():
        hrow_copy.wait()
        take_row(0)
        take_row(1)

    pl.semaphore_wait(barrier, n_row + n_col - 2)

    @pl.when(r == 0)
    def _():
        to_rows(rowc.at[0, 0:halves, 0:ut], row_sem.at[PAIRS + 1])
        to_rows(rowc.at[0, halves:2 * halves, 0:ut], row_sem.at[PAIRS + 2])
        to_rows(rowc.at[1, :, 0:ut], row_sem.at[0])

        @pl.when(c == 0)
        def _():
            phead[...] = headrows[:, 0:LANES]
            for dr in range(1, n_row):
                remote(headrows.at[:, 0:LANES], phead, head_sem, along_row(dr)).start()

    @pl.when(r != 0)
    def _():
        landed(rowc.at[0, 0:halves, 0:ut], row_sem.at[PAIRS + 1])

    def positions(n, base):
        shape = (n, up, LANES)
        t = lax.broadcasted_iota(jnp.int32, shape, 1)
        x = (lax.broadcasted_iota(jnp.int32, shape, 0) * ut + t) * LANES + lax.broadcasted_iota(jnp.int32, shape, 2)
        return jnp.where(t < ut, x + base, -2)

    l128 = lax.broadcasted_iota(jnp.int32, (1, LANES), 1)
    pos_r = positions(2, r * rows)
    pos_c = positions(2 * halves, c * cols)
    pos_h = jnp.where(lax.broadcasted_iota(jnp.int32, (1, SUB, LANES), 1) < 1,
                      lax.broadcasted_iota(jnp.int32, (1, SUB, LANES), 2), -2)
    k16 = lax.broadcasted_iota(jnp.int32, (K, LANES), 0)
    s40 = lax.broadcasted_iota(jnp.int32, (2 * K + SUB, LANES), 0)
    t40 = lax.broadcasted_iota(jnp.int32, (2 * K + SUB, LANES), 1)
    eye40 = s40 == t40
    diag3 = (lax.broadcasted_iota(jnp.int32, (GROUPS, SUB, LANES), 0) * SUB
             + lax.broadcasted_iota(jnp.int32, (GROUPS, SUB, LANES), 1)
             == lax.broadcasted_iota(jnp.int32, (GROUPS, SUB, LANES), 2))

    def srow(k):
        return scal[k:k + 1, :]

    def splat(ref, k, like):
        return jnp.broadcast_to(ref[k:k + 1, :], like.shape[1:])[None]

    def weighted(w, ref, like, sl=slice(None)):
        acc = w[0, sl] * splat(ref, 0, like)
        for k in range(1, 2 * K):
            acc = acc + w[k, sl] * splat(ref, k, like)
        return acc

    def record(j, w, c0, u, p, au_ref, au, c0n, pn, pos, sl=slice(None)):
        kap, e, inv = splat(scal, 1, pos), splat(scal, 2, pos), splat(scal, 3, pos)
        hot = jnp.where(j >= 0, j + 1, -1)
        u_old = u[sl]
        un = jnp.where(pos > j + 1, (c0[sl] + e * u_old) * inv, 0.0)
        un = jnp.where(pos == hot, 1.0, un)
        fixed = p[sl] - kap * u_old
        w[K + j - 1, sl] = fixed
        w[jnp.maximum(j, 0), sl] = un
        w[K + j, sl] = pn
        c0[sl] = c0n
        u[sl] = un
        p[sl] = pn
        au_ref[sl] = au

    def advance(j, w, c0, u, p, au_ref, au, row, pos):
        ta = splat(scal, 0, pos) * au
        c0n = row - ta + weighted(w, coefc, pos)
        pn = ta - weighted(w, coefp, pos)
        record(j, w, c0, u, p, au_ref, au, c0n, pn, pos)

    def finish(j, h, w, c0, u, p, au_ref, q, total, row, row_next, pos, b0):
        n = pos.shape[0] // 2
        sl = slice(h * n, (h + 1) * n)
        ps = pos[sl]
        tau, kap, e, inv, uj1 = (splat(scal, k, pos) for k in (0, 1, 2, 3, 5))
        nxt = row_next[sl]
        aq = au_ref[sl] - row[sl] - uj1 * nxt
        au = (total + e * aq) * inv + nxt
        pn = tau * au - weighted(w, coefp, pos, sl)
        c0n = q[sl] + (2.0 * kap * uj1) * u[sl] - pn
        record(j, w, c0, u, p, au_ref, au, c0n, pn, ps, sl)
        b0[sl] = jnp.where(ps > j + 2, c0n, 0.0)

    def fold(x):
        y = x.reshape(-1, SUB, LANES)
        acc = y[0]
        for k in range(1, y.shape[0]):
            acc = acc + y[k]
        return acc

    def prepare(w, u, p, b0):
        x = b0[...]
        for k in range(2 * K):
            dacc[k] = fold(w[k] * x)
        dacc[2 * K] = fold(x * x)
        dacc[2 * K + 1] = fold(u[...] * p[...])

    def dots_row():
        acc = jnp.zeros((SUB, LANES), F32)
        for k in range(2 * K + 2):
            s = jnp.sum(dacc[k], axis=1, keepdims=True)
            acc = jnp.where(jnp.broadcast_to(l128, (SUB, LANES)) == k, s, acc)
        return jnp.sum(acc, axis=0, keepdims=True)

    def matvec_cols(i, mid):
        def reduce_block(k, base):
            a = accs[block_rows(k), :].reshape(GROUPS, SUB, LANES)
            s = jnp.sum(a, axis=2, keepdims=True)
            row = jnp.sum(jnp.sum(jnp.where(diag3, s, 0.0), axis=0), axis=0, keepdims=True)
            sum_b[i, c, base, pl.ds(k - base * ut, 1), :] = row

        def products(k, h, xb):
            for g in range(0, GROUPS, BATCH):
                piece = pl.ds(pl.multiple_of(k * LANES + g * SUB, SUB), BATCH * SUB)
                shape = (BATCH, SUB, LANES)
                acc = jnp.zeros(shape, F32) if h == 0 else accs[piece, :].reshape(shape)
                for t in range(ht):
                    acc = acc + tile[piece, lanes_of(h * ht + t)].reshape(shape) * xb[t][None]
                accs[piece, :] = acc.reshape(BATCH * SUB, LANES)

        def wide_x(h):
            ts = [h * ht + t for t in range(ht)]
            return [jnp.broadcast_to(b0c[t // ut, t % ut:t % ut + 1, :], (SUB, LANES)) for t in ts]

        xa = wide_x(0)

        def pass0(q, carry):
            for s in range(STEP):
                pl.when(i == 0)(lambda s=s: chunk(q * STEP + s).wait())
            for s in range(STEP):
                products(q * STEP + s, 0, xa)
            return carry

        lax.fori_loop(0, blocks // STEP, pass0, 0)
        mid()
        xb = wide_x(1)
        turns = ut // STEP
        for a in range(2):
            def pass1(q, carry, a=a, dots=False):
                if dots:
                    sc_b[i, c] = dots_row()
                for s in range(STEP):
                    products(q * STEP + s, 1, xb)
                    if s > 0:
                        reduce_block(q * STEP + s - 1, a)
                return carry

            for q in range(turns):
                early = a == 0 and q == 0
                pass1(a * turns + q, 0, a, early)
                if early:
                    to_cols(sc_b.at[i, c], sb_sem.at[i])
                reduce_block((a * turns + q) * STEP + STEP - 1, a)
            to_cols(sum_b.at[i, c, a, 0:ut], yb_sem.at[i, a])

    def spread(k, a):
        xs[block_rows(k), :] = spread_row(b0r[a, pl.ds(k - a * ut, 1), :])

    def spread_first(a):
        for s in range(STEP):
            spread(a * ut + s, a)

    def matvec_rows(i, mid):
        zero = jnp.zeros((SUB, LANES), F32)

        def products(k, acc, base):
            out = list(acc)
            for g in range(GROUPS):
                piece = pl.ds(pl.multiple_of(k * LANES + g * SUB, SUB), SUB)
                b = xs[piece, :]
                for t in range(len(out)):
                    out[t] = out[t] + tile[piece, lanes_of(base + t)] * b
            return tuple(out)

        def ahead(k, a):
            spread(jnp.minimum(k, a * ut + ut - 1), a)

        def sweep(a, base, lead, dots=False):
            def body(q, acc):
                if dots:
                    sc_a[i, r] = dots_row()
                for s in range(STEP):
                    acc = products(q * STEP + s, acc, base)
                    if lead and s == 0:
                        for n in range(STEP - 1):
                            ahead(q * STEP + lead + n, a)
                    if lead and s == 1:
                        ahead(q * STEP + lead + STEP - 1, a)
                return acc
            return body

        turns = ut // STEP
        acc = lax.fori_loop(0, turns, sweep(0, 0, 1), (zero,) * ctiles)
        for t in range(ctiles):
            acca[t] = acc[t]
        mid()
        for h in range(2):
            acc = tuple(acca[h * ht + t] for t in range(ht))
            lead = STEP if h == 0 else 0
            if h == 0:
                cut = turns + jnp.minimum(i + 1, 1)
                acc = lax.fori_loop(turns, cut, sweep(1, 0, lead, True), acc)
                to_rows(sc_a.at[i, r], sa_sem.at[i])
                acc = lax.fori_loop(cut, 2 * turns, sweep(1, 0, lead), acc)
            else:
                acc = lax.fori_loop(turns, 2 * turns, sweep(1, h * ht, 0), acc)
            for t in range(ht):
                sum_a[i, r, h, t // ut, t % ut:t % ut + 1, :] = jnp.sum(acc[t], axis=0, keepdims=True)
            to_rows(sum_a.at[i, r, h, :, 0:ut], ya_sem.at[i, h])

    def head_advance(j, auh_row):
        advance(j, wh, c0h, uh, ph, auh, auh_row, phead[pl.ds(j + 1, 1), :][None] * jnp.ones((1, SUB, 1), F32), pos_h)

    def lane_pick(x, index):
        s = jnp.sum(jnp.where(l128 == index, x, 0.0), axis=1, keepdims=True)
        return jnp.broadcast_to(s, x.shape)

    def picks(j):
        head = wh[:, 0, 0, :]
        return (lane_pick(head, j), lane_pick(head, j + 1), lane_pick(c0h[0, 0:1, :], j + 1),
                lane_pick(uh[0, 0:1, :], j + 1), lane_pick(ph[0, 0:1, :], j))

    def pre_q(w, q, picked, row_next, pos):
        hj1 = picked[1]
        coefc[0:K, :] = hj1[K:2 * K]
        coefc[K:2 * K, :] = hj1[0:K]
        q[...] = row_next - weighted(w, coefc, pos)

    def scalars(j, sc, picked):
        hj, hj1, c0h1, uj1, pent = picked
        d = jnp.sum(jnp.where(eye40, jnp.broadcast_to(sc, eye40.shape), 0.0), axis=1, keepdims=True)
        d = jnp.broadcast_to(d, eye40.shape)
        vb, wb = d[0:K], d[K:2 * K]
        n0, kp = d[2 * K:2 * K + 1], d[2 * K + 1:2 * K + 2]
        hjv, hjw, hj1v, hj1w = hj[0:K], hj[K:2 * K], hj1[0:K], hj1[K:2 * K]
        last = k16 == j - 1
        tau_prev, bb_prev = srow(0), srow(4)
        kap = 0.5 * tau_prev * kp
        e = 2.0 * kap - pent
        lead = c0h1 + e * uj1
        n1 = jnp.sum(jnp.where(last, vb, 0.0), axis=0, keepdims=True)
        b2 = jnp.maximum(n0 + e * (2.0 * n1 + e * (bb_prev - uj1 * uj1)), 0.0)
        sig = jnp.sqrt(b2 + lead * lead)
        inv = 1.0 / (lead + sig)
        tau = 1.0 + lead / sig
        lk = jnp.where(last, kap, 0.0)
        hjw = hjw - lk * hjv
        hj1w = hj1w - lk * hj1v
        uu = bb_prev + 1.0
        vup = jnp.where(last, uu, vuwu[0:K, :])
        wup = jnp.where(last, kp - kap * uu, vuwu[K:2 * K, :])
        wb = wb - lk * vb
        vu = (vb + e * (vup - hjv - uj1 * hj1v)) * inv + hj1v
        wu = (wb + e * (wup - hjw - uj1 * hj1w)) * inv + hj1w
        beta = tau * vu - hj1v
        alpha = tau * wu - hj1w - lk * beta
        delta = tau * vu
        gamma = tau * wu - lk * delta
        coefc[0:K, :] = alpha
        coefc[K:2 * K, :] = beta
        coefp[0:K, :] = gamma
        coefp[K:2 * K, :] = delta
        vuwu[0:K, :] = vu
        vuwu[K:2 * K, :] = wu
        scal[0:1, :] = tau
        scal[1:2, :] = kap
        scal[2:3, :] = e
        scal[3:4, :] = inv
        scal[4:5, :] = b2 * inv * inv
        scal[5:6, :] = uj1
        coef[0:1, :] = jnp.where(l128 == j, tau, coef[0:1, :])
        coef[1:2, :] = jnp.where(l128 == j, -sig, coef[1:2, :])

    def slot_sum(read, n):
        acc = read(0)
        for s in range(1, n):
            acc = acc + read(s)
        return acc

    def flat(ref):
        n = ref.shape[0]
        return jnp.concatenate([ref[h, t:t + 1, :] for h in range(n) for t in range(ut)], axis=1)

    def send_v(k):
        vout[k, c] = wc[k]
        to_cols(vout.at[k, c, :, 0:ut], v_sem.at[k])

    def place_v(k):
        landed(vout.at[k, 0:n_col - 1, :, 0:ut], v_sem.at[k])
        refl[pl.ds(k, 1), :] = jnp.concatenate([flat(vout.at[k, s]) for s in range(n_col)], axis=1)

    def flat_v(k, w, out):
        out[pl.ds(k, 1), :] = flat(w.at[k])

    piece_c = pl.ds(own_half * 2, 2)

    def send_au_b(i):
        @pl.when(diag)
        def _():
            red_b[i] = auc[piece_c]
            to_cols(red_b.at[i, :, 0:ut], rb_sem.at[i])

    def send_rows_b(i):
        @pl.when(diag)
        def _():
            for q in range(2):
                row_b[i, q] = rowc[2 * i + q, piece_c]
            to_cols(row_b.at[i, :, :, 0:ut], wb_sem.at[i])

    def finish_cols(i, h):
        landed(sum_b.at[i, 0:n_col - 1, 0, 0:ut], yb_sem.at[i, h])
        finish(2 * i, h, wr, c0r, ur, pr, aur, qr, slot_sum(lambda s: sum_b[i, s, h:h + 1], n_col),
               row_b[i, 0], row_b[i, 1], pos_r, b0r)

    def finish_rows(i, h):
        landed(sum_a.at[i, 0:n_row - 1, 0, :, 0:ut], ya_sem.at[i, h])
        finish(2 * i + 1, h, wc, c0c, uc, pc, auc, qc, slot_sum(lambda s: sum_a[i, s, h], n_row),
               rowc[2 * i + 1], rowc[2 * i + 2], pos_c, b0c)

    def start_half(h):
        sl = slice(h * halves, (h + 1) * halves)
        x = rowc[0, sl]
        c0c[sl] = x
        b0c[sl] = jnp.where(pos_c[sl] > 1, x, 0.0)

    def step_cols(i):
        j = 2 * i

        def mid():
            @pl.when(i == 0)
            def _():
                @pl.when(r != 0)
                def _():
                    landed(rowc.at[0, 0:halves, 0:ut], row_sem.at[PAIRS + 2])
                    landed(rowc.at[1, :, 0:ut], row_sem.at[0])

                start_half(1)
                send_rows_b(0)

            pl.when(i > 0)(lambda: finish_rows(jnp.maximum(i - 1, 0), 1))
            prepare(wc, uc, pc, b0c)
            send_au_b(i)

            @pl.when(c == 0)
            def _():
                hd_b[i] = auc[0:1, 0:SUB]
                to_cols(hd_b.at[i], hb_sem.at[i])

                @pl.when(i == 0)
                def _():
                    pl.when(r != 0)(lambda: landed(phead, head_sem))
                    to_cols(phead, head_sem)

        matvec_cols(i, mid)

        @pl.when(r == 0)
        def _():
            take_row(j + 2)
            take_row(j + 3)
            to_rows(rowc.at[pl.ds(j + 2, 2), :, 0:ut], row_sem.at[i + 1])

        @pl.when(jnp.logical_and(i == 0, c != 0))
        def _():
            landed(phead, head_sem)

        pl.when(jnp.logical_not(diag))(lambda: landed(row_b.at[i, :, :, 0:ut], wb_sem.at[i]))
        pl.when(c != 0)(lambda: landed(hd_b.at[i], hb_sem.at[i]))
        head_advance(j - 1, hd_b[i])
        picked = picks(j)
        pl.when(jnp.logical_not(diag))(lambda: landed(red_b.at[i, :, 0:ut], rb_sem.at[i]))
        advance(j - 1, wr, c0r, ur, pr, aur, red_b[i], row_b[i, 0], pos_r)
        pre_q(wr, qr, picked, row_b[i, 1], pos_r)
        landed(sc_b.at[i, 0:n_col - 1], sb_sem.at[i])
        scalars(j, slot_sum(lambda s: sc_b[i, s], n_col), picked)
        finish_cols(i, 0)
        spread(0, 0)

    def step_rows(i):
        j = 2 * i + 1

        def mid():
            finish_cols(i, 1)
            spread_first(1)
            prepare(wr, ur, pr, b0r)

            @pl.when(diag)
            def _():
                red_a[i, own_half] = aur[...]
                to_rows(red_a.at[i, own_half, :, 0:ut], ra_sem.at[i, own_half])

            @pl.when(r == 0)
            def _():
                hd_a[i] = aur[0:1, 0:SUB]
                to_rows(hd_a.at[i], ha_sem.at[i])

        matvec_rows(i, mid)

        pl.when(i > 0)(lambda: place_v(jnp.maximum(2 * i - 2, 0)))
        pl.when(i > 1)(lambda: place_v(jnp.maximum(2 * i - 3, 0)))
        pl.when(i > 0)(lambda: send_v(jnp.maximum(2 * i - 1, 0)))
        pl.when(r != 0)(lambda: landed(rowc.at[0:2, :, 0:ut], row_sem.at[i + 1]))
        send_rows_b(i + 1)
        pl.when(r != 0)(lambda: landed(hd_a.at[i], ha_sem.at[i]))
        head_advance(j - 1, hd_a[i])
        picked = picks(j)
        for h in range(halves):
            pl.when(r != halves * c + h)(lambda h=h: landed(red_a.at[i, h, :, 0:ut], ra_sem.at[i, h]))
        advance(j - 1, wc, c0c, uc, pc, auc, jnp.concatenate([red_a[i, h] for h in range(halves)], axis=0),
                rowc[j], pos_c)
        send_v(j - 1)
        pre_q(wc, qc, picked, rowc[j + 1], pos_c)
        landed(sc_a.at[i, 0:n_row - 1], sa_sem.at[i])
        scalars(j, slot_sum(lambda s: sc_a[i, s], n_row), picked)
        finish_rows(i, 0)

    def pair(i, carry):
        step_cols(i)
        step_rows(i)
        return carry

    start_half(0)
    lax.fori_loop(0, PAIRS, pair, 0)

    f = PAIRS
    finish_rows(f - 1, 1)
    send_au_b(f)
    kp = jnp.sum(fold(uc[...] * pc[...]), axis=1, keepdims=True)
    sc_b[f, c] = jnp.sum(jnp.broadcast_to(kp, (SUB, LANES)), axis=0, keepdims=True)
    to_cols(sc_b.at[f, c], sb_sem.at[f])
    send_v(K - 1)
    for k in range(2 * K - 1):
        flat_v(k, wc, vwc)
    for k in range(2 * K - 2):
        if k != K - 1:
            flat_v(k, wr, vwr)
    place_v(K - 3)
    place_v(K - 2)
    def drain(i, carry):
        landed(sum_a.at[i, 0:n_row - 1, :, :, 0:ut], ssem)
        landed(sc_a.at[i, 0:n_row - 1], ssem)
        landed(sum_b.at[i, 0:n_col - 1, :, 0:ut], ssem)
        landed(sc_b.at[i, 0:n_col - 1], ssem)
        landed(vout.at[0:2, 0:n_col - 1, :, 0:ut], ssem)

        @pl.when(diag)
        def _():
            for dr in range(1, n_row):
                landed(red_a.at[i, 0, :, 0:ut], ssem)
            for dc in range(1, n_col):
                landed(red_b.at[i, :, 0:ut], ssem)
                landed(row_b.at[i, :, :, 0:ut], ssem)

        @pl.when(c == 0)
        def _():
            for dc in range(1, n_col):
                landed(hd_b.at[i], ssem)

        @pl.when(r == 0)
        def _():
            for dr in range(1, n_row):
                landed(hd_a.at[i], ssem)
                landed(rowc.at[0:2, :, 0:ut], ssem)
        return carry

    lax.fori_loop(0, PAIRS, drain, 0)
    pl.when(jnp.logical_not(diag))(lambda: landed(row_b.at[f, :, :, 0:ut], wb_sem.at[f]))
    pl.when(jnp.logical_not(diag))(lambda: landed(red_b.at[f, :, 0:ut], rb_sem.at[f]))
    advance(K - 1, wr, c0r, ur, pr, aur, red_b[f], row_b[f, 0], pos_r)
    flat_v(K - 1, wr, vwr)
    flat_v(2 * K - 2, wr, vwr)
    landed(sc_b.at[f, 0:n_col - 1], sb_sem.at[f])
    kap = 0.5 * srow(0) * slot_sum(lambda s: sc_b[f, s], n_col)
    wr[2 * K - 1] = pr[...] - jnp.broadcast_to(kap, (up, LANES))[None] * ur[...]
    wc[2 * K - 1] = pc[...] - jnp.broadcast_to(kap, (up, LANES))[None] * uc[...]
    flat_v(2 * K - 1, wr, vwr)
    flat_v(2 * K - 1, wc, vwc)
    place_v(K - 1)

    landed(sc_b.at[f, 0:n_col - 1], ssem)

    @pl.when(diag)
    def _():
        for dc in range(1, n_col):
            landed(red_b.at[f, :, 0:ut], ssem)
            landed(row_b.at[f, :, :, 0:ut], ssem)

    @pl.when(r == 0)
    def _():
        for dr in range(1, n_row):
            landed(rowc.at[0:2, :, 0:ut], ssem)

    @pl.when(c == 0)
    def _():
        for dc in range(1, n_col):
            landed(phead, ssem)

        @pl.when(r == 0)
        def _():
            for dr in range(1, n_row):
                landed(phead, ssem)


def pieces(x):
    hi = x.astype(jnp.bfloat16)
    rest = x - hi.astype(F32)
    mid = rest.astype(jnp.bfloat16)
    low = (rest - mid.astype(F32)).astype(jnp.bfloat16)
    return hi, mid, low


def update_kernel(rows, cols, tile, vwr, vwc, refl, coef, out, refl_out, coef_out, left, right, buf, sem, rsem):
    blocks = rows // LANES
    order = ((0, 0), (0, 1), (1, 0), (1, 1), (0, 2), (2, 0))
    two = 2 * K
    refl_copy = pltpu.make_async_copy(refl, refl_out, rsem)
    refl_copy.start()
    coef_out[...] = coef[:, 0:K]
    lp = pieces(vwr[...])
    wv = jnp.concatenate([vwc[K:two, :], vwc[0:K, :]], axis=0)
    rp = pieces(wv)
    for q, (a, b) in enumerate(order):
        left[q * two:(q + 1) * two, :] = lp[a]
        right[q * two:(q + 1) * two, :] = rp[b]

    def body(i, carry):
        part = pl.ds(pl.multiple_of(i * LANES, LANES), LANES)
        lt = left[:, part]
        change = lax.dot_general(lt, right[...], (((0,), (0,)), ((), ())), preferred_element_type=F32)
        buf[part, :] = tile[part, :] - change
        pltpu.make_async_copy(buf.at[part], out.at[part], sem).start()
        return carry

    lax.fori_loop(0, blocks, body, 0)
    pltpu.make_async_copy(buf, out, sem).wait()
    refl_copy.wait()


def make_per_device(n_row, n_col):
    def per_device(matrix):
        rows, cols = matrix.shape
        halves = cols // rows
        f32 = F32
        vmem = pl.BlockSpec(memory_space=pltpu.VMEM)
        anyspace = pl.BlockSpec(memory_space=pl.ANY)
        dma = pltpu.SemaphoreType.DMA
        full = n_row * rows
        up = tile_rows(rows // LANES // 2)

        def kernel(*refs):
            panel_kernel(rows, cols, n_row, n_col, *refs)

        def vm(*shape):
            return pltpu.VMEM(shape, f32)

        tile, refl, vwr, vwc, coef = pl.pallas_call(
            kernel,
            out_shape=(
                jax.ShapeDtypeStruct((rows, cols), f32),
                jax.ShapeDtypeStruct((K, full), f32),
                jax.ShapeDtypeStruct((2 * K, rows), f32),
                jax.ShapeDtypeStruct((2 * K, cols), f32),
                jax.ShapeDtypeStruct((2, LANES), f32),
            ),
            in_specs=[anyspace],
            out_specs=(vmem,) * 5,
            scratch_shapes=[
                vm(HEAD, cols), vm(HEAD, LANES), vm(K + 2, 2 * halves, up, LANES),
                vm(K, n_col, 2 * halves, up, LANES),
                vm(PAIRS, n_row, 2, halves, up, LANES), vm(PAIRS, n_col, 2, up, LANES),
                vm(PAIRS, n_row, 1, LANES), vm(PAIRS + 1, n_col, 1, LANES),
                vm(PAIRS, halves, 2, up, LANES), vm(PAIRS + 1, 2, up, LANES), vm(PAIRS + 1, 2, 2, up, LANES),
                vm(PAIRS, 1, SUB, LANES), vm(PAIRS, 1, SUB, LANES),
                vm(2 * K, 2, up, LANES), *[vm(2, up, LANES)] * 5,
                vm(2 * K, 2 * halves, up, LANES), *[vm(2 * halves, up, LANES)] * 5,
                vm(2 * K, 1, SUB, LANES), *[vm(1, SUB, LANES)] * 4,
                vm(2 * K, LANES), vm(2 * K, LANES), vm(2 * K, LANES), vm(8, LANES),
                vm(2, up, LANES), vm(2 * halves, up, LANES), vm(rows, LANES), vm(rows, LANES),
                vm(cols // LANES, SUB, LANES), vm(2 * K + 2, SUB, LANES),
                dma((rows // LANES,)), dma, dma, dma((PAIRS + 3,)), dma((K,)),
                dma((PAIRS, 2)), dma((PAIRS,)), dma((PAIRS, halves)), dma((PAIRS,)),
                dma((PAIRS, 2)), dma((PAIRS + 1,)), dma((PAIRS + 1,)), dma((PAIRS + 1,)), dma((PAIRS,)),
                dma,
            ],
            compiler_params=pltpu.CompilerParams(
                collective_id=0, has_side_effects=True, vmem_limit_bytes=24 * 1024 * 1024),
        )(matrix)

        def update(*refs):
            update_kernel(rows, cols, *refs)

        return pl.pallas_call(
            update,
            out_shape=(
                jax.ShapeDtypeStruct((rows, cols), f32),
                jax.ShapeDtypeStruct((K, full), f32),
                jax.ShapeDtypeStruct((2, K), f32),
            ),
            in_specs=[vmem] * 5,
            out_specs=(anyspace, anyspace, vmem),
            scratch_shapes=[
                pltpu.VMEM((12 * K, rows), jnp.bfloat16),
                pltpu.VMEM((12 * K, cols), jnp.bfloat16),
                vm(rows, cols),
                dma, dma,
            ],
            compiler_params=pltpu.CompilerParams(vmem_limit_bytes=24 * 1024 * 1024),
        )(tile, vwr, vwc, refl, coef)
    return per_device


def solution(mesh):
    return jax.shard_map(
        make_per_device(mesh.shape["row"], mesh.shape["col"]),
        mesh=mesh,
        in_specs=(P("row", "col"),),
        out_specs=(P("row", "col"), P(), P()),
        check_vma=False,
    )
```
